512 devices in a mesh: tm: 32 (over y, x, core), diag: 16 (over z).
Axes of the slice: x: 4, y: 4, z: 16, core: 2. Of those that a mesh axis runs over, the one named last changes fastest.
Arguments:
- series: float32 [524288], P('tm'), may hold values from -6 to 6
- tail: float32 [256], replicated, may hold values from -6 to 6
- diag_offsets: int32 [16], P('diag'), may hold values from 0 to 12000, as said below
- exclusion: int32 [1], replicated, may hold values from 64 to 255
Outputs:
- profile: float32 [524288], P(('tm', 'diag'))
The draws below stay inside these ranges and needn't reach their ends.
Inputs may be any that keep to these rules, and one draw needn't show every extreme that they name: `diag_offsets`: in every draw some group starts at 12000 and another below 64; the others anywhere in the range, blocks may intersect.
All inputs are finite; a program needn't handle non-finite values.
Results may differ from the reference program's by a relative error of at most 0.0003.
Values sent between devices are 32-bit elements; how exact they have to be, the bound alone decides.
A program may use at most 64 MiB of HBM per device.

```python
import jax
import jax.numpy as jnp
from jax import lax

M = 256
KB = 32
RB = 8192
REACH = 12288
SERIES = 524288
N_TM = 32
N_DIAG = 16


def draw_diag_offsets(key, part):
    highest = REACH - KB - M
    keys = jax.random.split(jax.random.fold_in(key, 17), 3)
    drawn = jax.random.randint(keys[0], (N_DIAG,), 0, highest + 1)
    chosen = jax.random.permutation(keys[1], N_DIAG)
    shallow = jax.random.randint(keys[2], (), 0, M // 4)
    group_ids = jnp.arange(N_DIAG)
    drawn = jnp.where(group_ids == chosen[0], highest, drawn)
    drawn = jnp.where(group_ids == chosen[1], shallow, drawn)
    return drawn.astype(jnp.int32)


def shard_levels(rng, extent, shards, smallest, top_value):
    def one(position, blocks):
        draws = jax.random.uniform(jax.random.fold_in(jax.random.fold_in(rng, 6), position), (blocks,), jnp.float32, smallest / len(shards), top_value / len(shards))
        return jnp.repeat(jnp.exp(draws), extent[position] // blocks).reshape((-1,) + (1,) * (len(extent) - position - 1))

    loudness = one(*shards[0])
    for cut in shards[1:]:
        loudness = loudness * one(*cut)
    return loudness


def gaussian(stream_key, dims, scale, most, cuts=(), held_as=jnp.bfloat16):
    values = jax.random.normal(stream_key, dims, jnp.float32) * scale
    if len(cuts) > 0:
        values = shard_levels(stream_key, dims, cuts, -0.22, 0.18) * values
    return jnp.clip(values, min=-most, max=most).astype(held_as)


def setup_inputs(seed: int = 0) -> dict:
    arg_keys = jax.random.split(jax.random.key(seed), 5)
    return {
        "series": gaussian(arg_keys[0], (SERIES,), 1.0, 6.0, ((0, 32),), jnp.float32),
        "tail": gaussian(arg_keys[1], (M,), 1.0, 6.0, (), jnp.float32),
        "diag_offsets": draw_diag_offsets(jax.random.fold_in(arg_keys[4], 71), 0),
        "exclusion": jax.random.randint(arg_keys[3], (1,), M // 4, M).astype(jnp.int32),
    }


FILL = 1e+30

def window_stats(extended):
    count = extended.shape[0] // M
    blocks = jnp.concatenate([extended, jnp.zeros((M,), jnp.float32)]).reshape(count + 1, M)
    row_ids = lax.broadcasted_iota(jnp.int32, (M, M), 0)
    col_ids = lax.broadcasted_iota(jnp.int32, (M, M), 1)
    upper = (row_ids >= col_ids).astype(jnp.float32)
    lower = (row_ids < col_ids).astype(jnp.float32)

    def window_sums(values):
        head = jnp.dot(values[:-1], upper, precision=lax.Precision.HIGHEST, preferred_element_type=jnp.float32)
        after = jnp.dot(values[1:], lower, precision=lax.Precision.HIGHEST, preferred_element_type=jnp.float32)
        return (head + after).reshape(-1)
    first = window_sums(blocks) / M
    second = window_sums(blocks * blocks) / M
    return (first, 1.0 / jnp.sqrt(second - first * first + 1e-05))

def hankel(vector, height, width):
    span = height + width
    tiled = jnp.tile(vector[:span], height + 1)[:height * (span + 1)]
    return tiled.reshape(height, span + 1)[:, :width]

def skew(matrix):
    height, width = matrix.shape
    padded = jnp.concatenate([matrix, jnp.full((height, height), FILL, matrix.dtype)], axis=1)
    flat = padded.reshape(-1)[:height * (width + height - 1)]
    return flat.reshape(height, width + height - 1)

def running_sums(values):
    height, width = values.shape
    inner = 128 if width % 128 == 0 else width
    grouped = values.reshape(height, width // inner, inner)
    within = jnp.cumsum(grouped, axis=2) - grouped
    totals = lax.optimization_barrier(jnp.sum(grouped, axis=2))
    before = jnp.cumsum(totals, axis=1) - totals
    return ((within + before[:, :, None]).reshape(height, width), lax.optimization_barrier(jnp.sum(totals, axis=1)))

def block_terms(extended, offset, row_start, rows):
    leading = lax.dynamic_slice_in_dim(extended, row_start, rows + M)
    partner = hankel(lax.dynamic_slice_in_dim(extended, row_start + offset, KB + rows + M), KB, rows + M)
    return leading[None, M:] * partner[:, M:] - leading[None, :rows] * partner[:, :rows]

def first_products(extended, offset):
    partner = hankel(lax.dynamic_slice_in_dim(extended, offset, KB + M), KB, M)
    return jnp.dot(partner, extended[:M], precision=lax.Precision.HIGHEST, preferred_element_type=jnp.float32)

def sweep(extended, means, spreads, offset, exclusion_width, limit, start, segment):
    rows = min(RB, segment)
    diag_ids = lax.broadcasted_iota(jnp.int32, (KB, rows), 0)
    row_ids = lax.broadcasted_iota(jnp.int32, (KB, rows), 1)

    def advance(index, carry):
        current, row_best, column_best = carry
        row_start = (index * rows).astype(jnp.int32)
        change = block_terms(extended, offset, row_start, rows)
        running, total = running_sums(change)
        products = current[:, None] + running
        mean_row = lax.dynamic_slice_in_dim(means, row_start, rows)
        spread_row = lax.dynamic_slice_in_dim(spreads, row_start, rows)
        mean_pair = hankel(lax.dynamic_slice_in_dim(means, row_start + offset, KB + rows), KB, rows)
        spread_pair = hankel(lax.dynamic_slice_in_dim(spreads, row_start + offset, KB + rows), KB, rows)
        corr = (products / M - mean_row[None, :] * mean_pair) * (spread_row[None, :] * spread_pair)
        distance = jnp.sqrt(1.0 - corr)
        partner_pos = row_start + offset + diag_ids + row_ids
        counted = (offset + diag_ids >= exclusion_width) & (partner_pos < limit)
        masked = jnp.where(counted, distance, FILL)
        row_best = lax.dynamic_update_slice_in_dim(row_best, lax.optimization_barrier(jnp.min(masked, axis=0)), row_start, 0)
        column_block = lax.optimization_barrier(jnp.min(skew(masked), axis=0))
        column_start = (row_start + offset).astype(jnp.int32)
        previous = lax.dynamic_slice_in_dim(column_best, column_start, rows + KB - 1)
        column_best = lax.dynamic_update_slice_in_dim(column_best, jnp.minimum(previous, column_block), column_start, 0)
        return (current + total, row_best, column_best)
    initial = (start, jnp.full((segment,), FILL, jnp.float32), jnp.full((extended.shape[0],), FILL, jnp.float32))
    result = lax.fori_loop(0, segment // rows, advance, initial)
    return (result[1], result[2])

def reference(series, tail, diag_offsets, exclusion):
    total_points = series.shape[0]
    segment = total_points // N_TM
    reach = segment // 2 + segment // 4
    padded_series = jnp.concatenate([series, tail, jnp.zeros((reach - M,), jnp.float32)])
    means, spreads = window_stats(padded_series)
    exclusion_width = exclusion[0].astype(jnp.int32)
    profile_best = jnp.full((total_points,), FILL, jnp.float32)
    for group in range(N_DIAG):
        offset = diag_offsets[group].astype(jnp.int32)

        def one_segment(place):
            begin = (place * segment).astype(jnp.int32)
            extended = lax.dynamic_slice_in_dim(padded_series, begin, segment + reach)
            local_means = lax.dynamic_slice_in_dim(means, begin, segment + reach)
            local_spreads = lax.dynamic_slice_in_dim(spreads, begin, segment + reach)
            limit = jnp.where(place == N_TM - 1, segment, segment + reach).astype(jnp.int32)
            start = first_products(extended, offset)
            row_best, column_best = sweep(extended, local_means, local_spreads, offset, exclusion_width, limit, start, segment)
            return (jnp.minimum(row_best, column_best[:segment]), column_best[segment:])
        owned, upper = lax.map(one_segment, jnp.arange(N_TM, dtype=jnp.int32))
        spilled = jnp.concatenate([jnp.full((1, reach), FILL, jnp.float32), upper[:-1]], axis=0)
        spilled = jnp.concatenate([spilled, jnp.full((N_TM, segment - reach), FILL, jnp.float32)], axis=1)
        profile_best = jnp.minimum(profile_best, jnp.minimum(owned, spilled).reshape(-1))
    return profile_best
```

```python
import functools

import jax
import jax.numpy as jnp
from jax import lax
from jax.experimental import pallas as pl
from jax.experimental.pallas import tpu as pltpu
from jax.sharding import PartitionSpec as P

F32 = jnp.float32
BF16 = jnp.bfloat16
MESH = pl.DeviceIdType.MESH

M = 256
KB = 32
LANES = 128
FILL = 1e30

HALO = 96
SEG = 128
OWN = 8
REGION = 2 * HALO + OWN + 16
EXT = 2 * HALO + SEG + 16
PRODUCT_BLOCKS = OWN + 2


def hop(k):
    return (k + 1) // 2 * (1 if k % 2 else -1)


def split2(v):
    high = v.astype(BF16)
    return high, (v - high.astype(F32)).astype(BF16)


def window_weights():
    r = lax.broadcasted_iota(jnp.int32, (256, 256), 0) & 127
    c = lax.broadcasted_iota(jnp.int32, (256, 256), 1)
    from_c = jnp.where(r >= c, 1.0, 0.0)
    before_c = jnp.where(r < c - 128, 1.0, 0.0)
    return jnp.where(c < 128, from_c, before_c).astype(BF16)


def window_stats(x_ref, w_ref, mean_ref, a_ref, b_ref):
    def window_sums(v):
        high, mid = split2(v)
        low = (v - high.astype(F32) - mid.astype(F32)).astype(BF16)
        g = jnp.dot(jnp.concatenate([high, mid], axis=1), w_ref[...], preferred_element_type=F32)
        g = g + jnp.dot(low, w_ref[:128, :], preferred_element_type=F32)
        from_c, before_c = g[:, :128], g[:, 128:]
        n = v.shape[0]
        return from_c[: n - 2] + (from_c + before_c)[1 : n - 1] + before_c[2:]

    x = x_ref[...]
    n = x.shape[0] - 2
    first = window_sums(x) * (1.0 / M)
    second = window_sums(x * x) * (1.0 / M)
    spread = 1.0 / jnp.sqrt(second - first * first + 1e-5)
    mean_ref[:n, :] = first
    a_ref[:n, :] = spread * (1.0 / M)
    b_ref[:n, :] = first * spread


def align(ref, z_ref, row, lane):
    n = z_ref.shape[0]
    shift = (128 - lane) & 127
    here = pltpu.roll(ref[pl.ds(row, n), :], shift, 1)
    after = pltpu.roll(ref[pl.ds(row + 1, n), :], shift, 1)
    lanes = lax.broadcasted_iota(jnp.int32, (n, 128), 1)
    z_ref[...] = jnp.where(lanes < 128 - lane, here, after)


def hankel(z_ref, blocks, emit):
    lanes = lax.broadcasted_iota(jnp.int32, (KB, 128), 1)
    subs = lax.broadcasted_iota(jnp.int32, (KB, 128), 0)
    keep = lanes < 97 + subs
    last = None
    for j in range(blocks + 1):
        rolled = pltpu.roll(
            jnp.broadcast_to(z_ref[j : j + 1, :], (KB, 128)), 97, 1, stride=1, stride_axis=0
        )
        if last is not None:
            emit(j - 1, jnp.where(keep, last, rolled))
        last = rolled


def band(beta, exclusion, pos0, total, x_ref, a_ref, b_ref, mean_ref, w_ref, zx, za, zb, lhs, sums, best):
    start = HALO * 128 + beta
    row = lax.shift_right_arithmetic(start, 7)
    lane = start & 127
    align(x_ref, zx, row, lane)
    align(a_ref, za, row, lane)
    align(b_ref, zb, row, lane)

    def own_row(ref, j):
        return jnp.broadcast_to(ref[HALO + j : HALO + j + 1, :], (KB, 128))

    def emit_products(j, y):
        high, low = split2(y * own_row(x_ref, j))
        lhs[KB * j : KB * j + KB, :128] = high
        lhs[KB * j : KB * j + KB, 128:] = low

    hankel(zx, PRODUCT_BLOCKS, emit_products)
    sums[...] = jnp.dot(lhs[...], w_ref[...], preferred_element_type=F32)

    delta = beta + 31 - lax.broadcasted_iota(jnp.int32, (KB, 128), 0)
    far = jnp.abs(delta) >= exclusion
    partner = pos0 + delta + lax.broadcasted_iota(jnp.int32, (KB, 128), 1)
    scaled = {}
    hankel(za, OWN, scaled.__setitem__)

    def emit_scores(j, y):
        here = slice(KB * j, KB * j + KB)
        middle = slice(KB * (j + 1), KB * (j + 2))
        ahead = slice(KB * (j + 2), KB * (j + 3))
        products = sums[here, :128] + (sums[middle, :128] + sums[middle, 128:]) + sums[ahead, 128:]
        score = products * scaled[j] - own_row(mean_ref, j) * y
        there = partner + 128 * j
        counted = far & (there >= 0) & (there < total)
        best[here, :] = jnp.maximum(best[here, :], jnp.where(counted, score, -FILL))

    hankel(zb, OWN, emit_scores)


def finish(best, a_ref, out_ref):
    rows = [jnp.max(best[KB * j : KB * j + KB, :], axis=0, keepdims=True) for j in range(OWN)]
    top = jnp.concatenate(rows, axis=0)
    corr = top * (a_ref[HALO : HALO + OWN, :] * float(M))
    out_ref[...] = jnp.where(top < -0.1 * FILL, FILL, jnp.sqrt(1.0 - corr))


def kernel(
    series, tail, offset, exclusion, out,
    ext, x_ref, mean_ref, a_ref, b_ref, w_ref, zx, za, zb, lhs, sums, best,
    mine, gathered, halo_send, halo_recv, off_send, off_recv,
    *, n_tm, n_diag, total,
):
    tm = lax.axis_index("tm")
    z = lax.axis_index("diag")
    has_prev = tm > 0
    has_next = tm < n_tm - 1

    def peer(h):
        return (tm, lax.rem(z + h + n_diag, n_diag))

    barrier = pltpu.get_barrier_semaphore()

    @pl.when(has_prev)
    def _():
        pl.semaphore_signal(barrier, inc=1, device_id=(tm - 1, z), device_id_type=MESH)

    @pl.when(has_next)
    def _():
        pl.semaphore_signal(barrier, inc=1, device_id=(tm + 1, z), device_id_type=MESH)

    for k in range(n_diag - 1, 0, -1):
        pl.semaphore_signal(barrier, inc=1, device_id=peer(hop(k)), device_id_type=MESH)

    mine[0, 0] = offset[0]
    gathered[0, 0] = offset[0]
    ext[HALO : HALO + SEG, :] = series[...]
    ext[2 * HALO + SEG :, :] = jnp.zeros((EXT - 2 * HALO - SEG, 128), F32)
    w_ref[...] = window_weights()
    best[...] = jnp.full(best.shape, -FILL, F32)

    @pl.when(jnp.logical_not(has_prev))
    def _():
        ext[:HALO, :] = jnp.zeros((HALO, 128), F32)

    @pl.when(jnp.logical_not(has_next))
    def _():
        ext[HALO + SEG : HALO + SEG + 2, :] = tail[...]
        ext[HALO + SEG + 2 : 2 * HALO + SEG, :] = jnp.zeros((HALO - 2, 128), F32)

    edge = has_prev.astype(jnp.int32) + has_next.astype(jnp.int32)
    pl.semaphore_wait(barrier, n_diag - 1 + edge)

    def offset_copy(k):
        return pltpu.make_async_remote_copy(
            mine, gathered.at[pl.ds(k, 1)], off_send.at[k], off_recv.at[k],
            device_id=peer(-hop(k)), device_id_type=MESH,
        )

    to_prev = pltpu.make_async_remote_copy(
        series.at[pl.ds(0, HALO)], ext.at[pl.ds(HALO + SEG, HALO)], halo_send.at[0], halo_recv.at[0],
        device_id=(tm - 1, z), device_id_type=MESH,
    )
    to_next = pltpu.make_async_remote_copy(
        series.at[pl.ds(SEG - HALO, HALO)], ext.at[pl.ds(0, HALO)], halo_send.at[1], halo_recv.at[1],
        device_id=(tm + 1, z), device_id_type=MESH,
    )

    for k in range(n_diag - 1, 0, -1):
        offset_copy(k).start()

    @pl.when(has_prev)
    def _():
        to_prev.start()

    @pl.when(has_next)
    def _():
        to_next.start()

    @pl.when(has_next)
    def _():
        to_prev.wait_recv()

    @pl.when(has_prev)
    def _():
        to_next.wait_recv()

    x_ref[...] = ext[pl.ds(pl.multiple_of(OWN * z, OWN), REGION), :]
    window_stats(x_ref, w_ref, mean_ref, a_ref, b_ref)
    pos0 = (tm * SEG + z * OWN) * 128

    def group(k, carry):
        @pl.when(k > 0)
        def _():
            pltpu.make_async_remote_copy(
                mine, gathered.at[pl.ds(k, 1)], off_send.at[k], off_recv.at[k],
                device_id=peer(1), device_id_type=MESH,
            ).wait_recv()

        first = gathered[k, 0]

        def side(d, c):
            beta = first + d * (-2 * first - (KB - 1))
            band(
                beta, exclusion[0], pos0, total,
                x_ref, a_ref, b_ref, mean_ref, w_ref, zx, za, zb, lhs, sums, best,
            )
            return c

        return lax.fori_loop(0, 2, side, carry)

    lax.fori_loop(0, n_diag, group, 0)
    finish(best, a_ref, out)

    for k in range(1, n_diag):
        offset_copy(k).wait_send()

    @pl.when(has_prev)
    def _():
        to_prev.wait_send()

    @pl.when(has_next)
    def _():
        to_next.wait_send()


def solution(mesh):
    n_tm, n_diag = mesh.shape["tm"], mesh.shape["diag"]

    def on_device(series, tail, diag_offsets, exclusion):
        total = series.shape[0] * n_tm
        vmem = pl.BlockSpec(memory_space=pltpu.VMEM)
        smem = pl.BlockSpec(memory_space=pltpu.SMEM)
        rows = pl.pallas_call(
            functools.partial(kernel, n_tm=n_tm, n_diag=n_diag, total=total),
            out_shape=jax.ShapeDtypeStruct((OWN, 128), F32),
            in_specs=[vmem, vmem, smem, smem],
            out_specs=vmem,
            scratch_shapes=[
                pltpu.VMEM((EXT, 128), F32),
                pltpu.VMEM((REGION, 128), F32),
                pltpu.VMEM((REGION, 128), F32),
                pltpu.VMEM((REGION, 128), F32),
                pltpu.VMEM((REGION, 128), F32),
                pltpu.VMEM((256, 256), BF16),
                pltpu.VMEM((16, 128), F32),
                pltpu.VMEM((16, 128), F32),
                pltpu.VMEM((16, 128), F32),
                pltpu.VMEM((KB * PRODUCT_BLOCKS, 256), BF16),
                pltpu.VMEM((KB * PRODUCT_BLOCKS, 256), F32),
                pltpu.VMEM((KB * OWN, 128), F32),
                pltpu.SMEM((1, 128), jnp.int32),
                pltpu.SMEM((16, 128), jnp.int32),
                pltpu.SemaphoreType.DMA((2,)),
                pltpu.SemaphoreType.DMA((2,)),
                pltpu.SemaphoreType.DMA((16,)),
                pltpu.SemaphoreType.DMA((16,)),
            ],
            compiler_params=pltpu.CompilerParams(collective_id=0, has_side_effects=True),
            name="profile_rows",
        )(
            series.reshape(SEG, 128),
            tail.reshape(M // 128, 128),
            diag_offsets,
            exclusion,
        )
        return rows.reshape(-1)

    in_specs = (P("tm"), P(), P("diag"), P())
    out_specs = P(("tm", "diag"))
    return jax.shard_map(
        on_device, mesh=mesh, in_specs=in_specs, out_specs=out_specs, check_vma=False
    )
```

```python
import functools

import jax
import jax.numpy as jnp
from jax import lax
from jax.experimental import pallas as pl
from jax.experimental.pallas import tpu as pltpu
from jax.sharding import PartitionSpec as P

F32 = jnp.float32
BF16 = jnp.bfloat16
MESH = pl.DeviceIdType.MESH

M = 256
KB = 32
LANES = 128
FILL = 1e30

HALO = 96
SEG = 128
OWN = 8
REGION = 2 * HALO + OWN + 16
SKEWED = REGION - 8
EXT = 2 * HALO + SEG + 16
STEPS = KB // 8
SCORE_BLOCKS = OWN + 1
NEAR = 4


def hop(k):
    return (k + 1) // 2 * (1 if k % 2 else -1)


def split2(v):
    high = v.astype(BF16)
    return high, (v - high.astype(F32)).astype(BF16)


def window_weights():
    r = lax.broadcasted_iota(jnp.int32, (256, 256), 0) & 127
    c = lax.broadcasted_iota(jnp.int32, (256, 256), 1)
    from_c = jnp.where(r >= c, 1.0, 0.0)
    before_c = jnp.where(r < c - 128, 1.0, 0.0)
    return jnp.where(c < 128, from_c, before_c).astype(BF16)


def window_stats(x_ref, w_ref, mean_ref, a_ref, b_ref):
    def window_sums(v):
        high, mid = split2(v)
        low = (v - high.astype(F32) - mid.astype(F32)).astype(BF16)
        g = jnp.dot(jnp.concatenate([high, mid], axis=1), w_ref[...], preferred_element_type=F32)
        g = g + jnp.dot(low, w_ref[:128, :], preferred_element_type=F32)
        from_c, before_c = g[:, :128], g[:, 128:]
        n = v.shape[0]
        return from_c[: n - 2] + (from_c + before_c)[1 : n - 1] + before_c[2:]

    x = x_ref[...]
    n = x.shape[0] - 2
    first = window_sums(x) * (1.0 / M)
    second = window_sums(x * x) * (1.0 / M)
    spread = 1.0 / jnp.sqrt(second - first * first + 1e-5)
    mean_ref[:n, :] = first
    a_ref[:n, :] = spread * (1.0 / M)
    b_ref[:n, :] = first * spread


def own_rows(ref, out_ref):
    n = 16
    here = ref[HALO : HALO + n, :]
    before = ref[HALO - 1 : HALO - 1 + n, :]
    lanes = lax.broadcasted_iota(jnp.int32, (n, 128), 1)
    out_ref[:n, :] = here
    for v in range(1, STEPS):
        shift = 8 * v
        out_ref[n * v : n * v + n, :] = jnp.where(
            lanes < shift, pltpu.roll(before, shift, 1), pltpu.roll(here, shift, 1)
        )


def skewed(pairs):
    lanes = lax.broadcasted_iota(jnp.int32, (8, 128), 1)
    subs = lax.broadcasted_iota(jnp.int32, (8, 128), 0)
    here = lanes < 121 + subs
    batch = SKEWED // 4

    def rows(i, carry):
        start = batch * i
        for ref, out_ref in pairs:
            last = None
            for j in range(batch + 1):
                row = jnp.broadcast_to(ref[pl.ds(start + j, 1), :], (8, 128))
                rolled = pltpu.roll(row, 121, 1, stride=1, stride_axis=0)
                if j:
                    out_ref[pl.ds(pl.multiple_of(8 * (start + j - 1), 8), 8), :] = jnp.where(here, last, rolled)
                last = rolled
        return carry

    lax.fori_loop(0, SKEWED // batch, rows, 0)


def hankel(ref, row, lane, blocks, emit):
    lanes = lax.broadcasted_iota(jnp.int32, (8, 128), 1)
    here = lanes < 128 - lane
    shift = (128 - lane) & 127
    rolled = [
        pltpu.roll(ref[pl.ds(8 * row + 8 * j, 8), :], shift, 1) for j in range(blocks + 1)
    ]
    for j in range(blocks):
        emit(j, jnp.where(here, rolled[j], rolled[j + 1]))


def group_scores(
    first, exclusion, pos0, total, x_ref, a_ref, b_ref, own_x, own_mean, w_ref, scratch, best
):
    subs = lax.broadcasted_iota(jnp.int32, (8, 128), 0)
    lanes = lax.broadcasted_iota(jnp.int32, (8, 128), 1)

    def rows_of(ref, v, j):
        return jnp.broadcast_to(ref[16 * v + j : 16 * v + j + 1, :], (8, 128))

    def at(j, v):
        return slice((STEPS * j + v) * 8, (STEPS * j + v) * 8 + 8)

    sides = []
    for side, (lhs, sums) in enumerate(scratch):
        beta = first if side == 0 else -first - (KB - 1)
        start = HALO * 128 + beta
        row = lax.shift_right_arithmetic(start, 7)
        lane = start & 127
        sides.append((side, beta, row, lane, lhs, sums))

    for _, _, row, lane, lhs, _ in sides:

        def emit_products(j, y, lhs=lhs):
            for v in range(STEPS):
                p = y * rows_of(own_x, v, j)
                lhs[at(j, v), :128] = p
                lhs[at(j, v), 128:] = p - p.astype(BF16).astype(F32)

        hankel(x_ref, row, lane, SCORE_BLOCKS + 2, emit_products)

    for _, _, _, _, lhs, sums in sides:
        sums[...] = jnp.dot(lhs[...], w_ref[...], preferred_element_type=F32)

    for side, beta, row, lane, _, sums in sides:
        partner = pos0 + beta + 7 - subs + lanes
        distance = beta + 7 - subs
        far = [
            (distance + 8 * v >= exclusion) if side == 0 else (-8 * v - distance >= exclusion)
            for v in range(STEPS)
        ]
        scaled = {}
        hankel(a_ref, row, lane, SCORE_BLOCKS, scaled.__setitem__)

        def emit_scores(j, y, side=side, sums=sums, partner=partner, scaled=scaled, far=far):
            inside = partner < total - 128 * j if side == 0 else partner >= -128 * j
            for v in range(STEPS):
                middle = at(j + 1, v)
                products = (
                    sums[at(j, v), :128] + (sums[middle, :128] + sums[middle, 128:]) + sums[at(j + 2, v), 128:]
                )
                score = products * scaled[j] - rows_of(own_mean, v, j) * y
                here = at(j, v)
                best[here, :] = jnp.maximum(best[here, :], jnp.where(inside & far[v], score, -FILL))

        hankel(b_ref, row, lane, SCORE_BLOCKS, emit_scores)


def finish(best, a_ref, out_ref):
    def part(j, v):
        return best[(STEPS * j + v) * 8 : (STEPS * j + v) * 8 + 8, :]

    lanes = lax.broadcasted_iota(jnp.int32, (8, 128), 1)
    tops = [part(j, 0) for j in range(OWN)]
    for v in range(1, STEPS):
        moved = [pltpu.roll(part(j, v), 128 - 8 * v, 1) for j in range(SCORE_BLOCKS)]
        for j in range(OWN):
            tops[j] = jnp.maximum(tops[j], jnp.where(lanes < 128 - 8 * v, moved[j], moved[j + 1]))
    top = jnp.concatenate([jnp.max(t, axis=0, keepdims=True) for t in tops], axis=0)
    corr = top * (a_ref[HALO : HALO + OWN, :] * float(M))
    out_ref[...] = jnp.where(top < -0.1 * FILL, FILL, jnp.sqrt(1.0 - corr))


def kernel(
    series, tail, offset, exclusion, out,
    ext, x_ref, mean_ref, a_ref, b_ref, w_ref, ones_ref,
    x_skew, a_skew, b_skew, own_x, own_mean, lhs0, sums0, lhs1, sums1, best,
    mine, gathered, halo_send, halo_recv, off_send, off_recv,
    *, n_tm, n_diag, total,
):
    tm = lax.axis_index("tm")
    z = lax.axis_index("diag")
    has_prev = tm > 0
    has_next = tm < n_tm - 1

    def peer(h):
        return (tm, lax.rem(z + h + n_diag, n_diag))

    barrier = pltpu.get_barrier_semaphore()

    @pl.when(has_prev)
    def _():
        pl.semaphore_signal(barrier, inc=1, device_id=(tm - 1, z), device_id_type=MESH)

    @pl.when(has_next)
    def _():
        pl.semaphore_signal(barrier, inc=1, device_id=(tm + 1, z), device_id_type=MESH)

    for k in range(2 * NEAR, 0, -1):
        pl.semaphore_signal(barrier, inc=1, device_id=peer(hop(k)), device_id_type=MESH)

    mine[0, 0] = offset[0]
    gathered[0, 0] = offset[0]
    ext[HALO : HALO + SEG, :] = series[...]
    ext[2 * HALO + SEG :, :] = jnp.zeros((EXT - 2 * HALO - SEG, 128), F32)
    w_ref[...] = window_weights()
    ones_ref[...] = w_ref[...].astype(F32)
    scratch = ((lhs0, sums0), (lhs1, sums1))
    best[...] = jnp.full(best.shape, -FILL, F32)

    @pl.when(jnp.logical_not(has_prev))
    def _():
        ext[:HALO, :] = jnp.zeros((HALO, 128), F32)

    @pl.when(jnp.logical_not(has_next))
    def _():
        ext[HALO + SEG : HALO + SEG + 2, :] = tail[...]
        ext[HALO + SEG + 2 : 2 * HALO + SEG, :] = jnp.zeros((HALO - 2, 128), F32)

    edge = has_prev.astype(jnp.int32) + has_next.astype(jnp.int32)
    pl.semaphore_wait(barrier, 2 * NEAR + edge)

    def offset_copy(k):
        h = hop(k)
        near = abs(h) <= NEAR
        source = mine if near else gathered.at[pl.ds(k - 2 * NEAR, 1)]
        to = -h if near else (-NEAR if h > 0 else NEAR)
        return pltpu.make_async_remote_copy(
            source, gathered.at[pl.ds(k, 1)], off_send.at[k], off_recv.at[k],
            device_id=peer(to), device_id_type=MESH,
        )

    to_prev = pltpu.make_async_remote_copy(
        series.at[pl.ds(0, HALO)], ext.at[pl.ds(HALO + SEG, HALO)], halo_send.at[0], halo_recv.at[0],
        device_id=(tm - 1, z), device_id_type=MESH,
    )
    to_next = pltpu.make_async_remote_copy(
        series.at[pl.ds(SEG - HALO, HALO)], ext.at[pl.ds(0, HALO)], halo_send.at[1], halo_recv.at[1],
        device_id=(tm + 1, z), device_id_type=MESH,
    )

    for k in range(2 * NEAR, 0, -1):
        offset_copy(k).start()

    @pl.when(has_prev)
    def _():
        to_prev.start()

    @pl.when(has_next)
    def _():
        to_next.start()

    for k in range(1, 2 * NEAR + 1):
        offset_copy(k).wait_recv()
        if k + 2 * NEAR < n_diag:
            offset_copy(k + 2 * NEAR).start()

    @pl.when(has_next)
    def _():
        to_prev.wait_recv()

    @pl.when(has_prev)
    def _():
        to_next.wait_recv()

    x_ref[...] = ext[pl.ds(pl.multiple_of(OWN * z, OWN), REGION), :]
    window_stats(x_ref, w_ref, mean_ref, a_ref, b_ref)
    skewed(((x_ref, x_skew), (a_ref, a_skew), (b_ref, b_skew)))
    own_rows(x_ref, own_x)
    own_rows(mean_ref, own_mean)
    pos0 = (tm * SEG + z * OWN) * 128

    def group(k, carry):
        @pl.when(k > 2 * NEAR)
        def _():
            pltpu.make_async_remote_copy(
                mine, gathered.at[pl.ds(k, 1)], off_send.at[k], off_recv.at[k],
                device_id=peer(1), device_id_type=MESH,
            ).wait_recv()

        first = gathered[k, 0]

        group_scores(
            first, exclusion[0], pos0, total,
            x_skew, a_skew, b_skew, own_x, own_mean, ones_ref, scratch, best,
        )
        return carry

    lax.fori_loop(0, n_diag, group, 0)
    finish(best, a_ref, out)

    for k in range(1, n_diag):
        offset_copy(k).wait_send()

    @pl.when(has_prev)
    def _():
        to_prev.wait_send()

    @pl.when(has_next)
    def _():
        to_next.wait_send()


def solution(mesh):
    n_tm, n_diag = mesh.shape["tm"], mesh.shape["diag"]

    def on_device(series, tail, diag_offsets, exclusion):
        total = series.shape[0] * n_tm
        vmem = pl.BlockSpec(memory_space=pltpu.VMEM)
        smem = pl.BlockSpec(memory_space=pltpu.SMEM)
        product_rows = KB * (SCORE_BLOCKS + 2)
        side_scratch = [pltpu.VMEM((product_rows, 256), F32)] * 2
        rows = pl.pallas_call(
            functools.partial(kernel, n_tm=n_tm, n_diag=n_diag, total=total),
            out_shape=jax.ShapeDtypeStruct((OWN, 128), F32),
            in_specs=[vmem, vmem, smem, smem],
            out_specs=vmem,
            scratch_shapes=[
                pltpu.VMEM((EXT, 128), F32),
                pltpu.VMEM((REGION, 128), F32),
                pltpu.VMEM((REGION, 128), F32),
                pltpu.VMEM((REGION, 128), F32),
                pltpu.VMEM((REGION, 128), F32),
                pltpu.VMEM((256, 256), BF16),
                pltpu.VMEM((256, 256), F32),
                pltpu.VMEM((8 * SKEWED, 128), F32),
                pltpu.VMEM((8 * SKEWED, 128), F32),
                pltpu.VMEM((8 * SKEWED, 128), F32),
                pltpu.VMEM((16 * STEPS, 128), F32),
                pltpu.VMEM((16 * STEPS, 128), F32),
                *side_scratch,
                *side_scratch,
                pltpu.VMEM((KB * SCORE_BLOCKS, 128), F32),
                pltpu.SMEM((1, 128), jnp.int32),
                pltpu.SMEM((16, 128), jnp.int32),
                pltpu.SemaphoreType.DMA((2,)),
                pltpu.SemaphoreType.DMA((2,)),
                pltpu.SemaphoreType.DMA((16,)),
                pltpu.SemaphoreType.DMA((16,)),
            ],
            compiler_params=pltpu.CompilerParams(collective_id=0, has_side_effects=True),
            name="profile_rows",
        )(
            series.reshape(SEG, 128),
            tail.reshape(M // 128, 128),
            diag_offsets,
            exclusion,
        )
        return rows.reshape(-1)

    in_specs = (P("tm"), P(), P("diag"), P())
    out_specs = P(("tm", "diag"))
    return jax.shard_map(
        on_device, mesh=mesh, in_specs=in_specs, out_specs=out_specs, check_vma=False
    )
```

```python
import functools

import jax
import jax.numpy as jnp
from jax import lax
from jax.experimental import pallas as pl
from jax.experimental.pallas import tpu as pltpu
from jax.sharding import PartitionSpec as P

F32 = jnp.float32
BF16 = jnp.bfloat16
MESH = pl.DeviceIdType.MESH

M = 256
KB = 32
LANES = 128
FILL = 1e30
NOWHERE = 1 << 30

HALO = 96
SEG = 128
OWN = 8
REGION = 2 * HALO + OWN + 16
SKEWED = REGION - 8
EXT = 2 * HALO + SEG + 16
STEPS = KB // 8
SCORE_BLOCKS = OWN + 1
NEAR = 4


def hop(k):
    return (k + 1) // 2 * (1 if k % 2 else -1)


def split2(v):
    high = v.astype(BF16)
    return high, (v - high.astype(F32)).astype(BF16)


def window_weights():
    r = lax.broadcasted_iota(jnp.int32, (256, 256), 0) & 127
    c = lax.broadcasted_iota(jnp.int32, (256, 256), 1)
    from_c = jnp.where(r >= c, 1.0, 0.0)
    before_c = jnp.where(r < c - 128, 1.0, 0.0)
    return jnp.where(c < 128, from_c, before_c).astype(BF16)


def window_stats(x_ref, w_ref, mean_ref, a_ref, b_ref):
    def window_sums(v):
        high, mid = split2(v)
        low = (v - high.astype(F32) - mid.astype(F32)).astype(BF16)
        g = jnp.dot(jnp.concatenate([high, mid], axis=1), w_ref[...], preferred_element_type=F32)
        g = g + jnp.dot(low, w_ref[:128, :], preferred_element_type=F32)
        from_c, before_c = g[:, :128], g[:, 128:]
        n = v.shape[0]
        return from_c[: n - 2] + (from_c + before_c)[1 : n - 1] + before_c[2:]

    x = x_ref[...]
    n = x.shape[0] - 2
    first = window_sums(x) * (1.0 / M)
    second = window_sums(x * x) * (1.0 / M)
    spread = 1.0 / jnp.sqrt(second - first * first + 1e-5)
    mean_ref[:n, :] = first
    a_ref[:n, :] = spread * (1.0 / M)
    b_ref[:n, :] = first * spread


def own_rows(ref, out_ref):
    n = 16
    here = ref[HALO : HALO + n, :]
    before = ref[HALO - 1 : HALO - 1 + n, :]
    lanes = lax.broadcasted_iota(jnp.int32, (n, 128), 1)
    out_ref[:n, :] = here
    for v in range(1, STEPS):
        shift = 8 * v
        out_ref[n * v : n * v + n, :] = jnp.where(
            lanes < shift, pltpu.roll(before, shift, 1), pltpu.roll(here, shift, 1)
        )


def skewed(pairs):
    lanes = lax.broadcasted_iota(jnp.int32, (8, 128), 1)
    subs = lax.broadcasted_iota(jnp.int32, (8, 128), 0)
    here = lanes < 121 + subs
    batch = SKEWED // 4

    def rows(i, carry):
        start = batch * i
        for ref, out_ref in pairs:
            last = None
            for j in range(batch + 1):
                row = jnp.broadcast_to(ref[pl.ds(start + j, 1), :], (8, 128))
                rolled = pltpu.roll(row, 121, 1, stride=1, stride_axis=0)
                if j:
                    out_ref[pl.ds(pl.multiple_of(8 * (start + j - 1), 8), 8), :] = jnp.where(here, last, rolled)
                last = rolled
        return carry

    lax.fori_loop(0, SKEWED // batch, rows, 0)


def hankel(ref, row, lane, blocks, emit):
    lanes = lax.broadcasted_iota(jnp.int32, (8, 128), 1)
    here = lanes < 128 - lane
    shift = (128 - lane) & 127
    rolled = [
        pltpu.roll(ref[pl.ds(8 * row + 8 * j, 8), :], shift, 1) for j in range(blocks + 1)
    ]
    for j in range(blocks):
        emit(j, jnp.where(here, rolled[j], rolled[j + 1]))


def group_scores(
    firsts, exclusion, pos0, total, x_ref, a_ref, b_ref, own_x, own_mean, w_ref, scratch, best
):
    subs = lax.broadcasted_iota(jnp.int32, (8, 128), 0)
    lanes = lax.broadcasted_iota(jnp.int32, (8, 128), 1)

    def rows_of(ref, v, j):
        return jnp.broadcast_to(ref[16 * v + j : 16 * v + j + 1, :], (8, 128))

    def at(j, v):
        return slice((STEPS * j + v) * 8, (STEPS * j + v) * 8 + 8)

    sides = []
    for first in firsts:
        for ahead in (True, False):
            beta = first if ahead else -first - (KB - 1)
            start = HALO * 128 + beta
            sides.append((ahead, beta, lax.shift_right_arithmetic(start, 7), start & 127))

    for (_, _, row, lane), (lhs, _) in zip(sides, scratch):

        def emit_products(j, y, lhs=lhs):
            own = jnp.concatenate([rows_of(own_x, v, j) for v in range(STEPS)], axis=0)
            p = jnp.concatenate([y] * STEPS, axis=0) * own
            lhs[KB * j : KB * j + KB, :128] = p
            lhs[KB * j : KB * j + KB, 128:] = p - p.astype(BF16).astype(F32)

        hankel(x_ref, row, lane, SCORE_BLOCKS + 2, emit_products)

    for lhs, sums in scratch[: len(sides)]:
        sums[...] = jnp.dot(lhs[...], w_ref[...], preferred_element_type=F32)

    masks, scaled, shifted = [], [], []
    for ahead, beta, row, lane in sides:
        distance = beta + 7 - subs
        masks.append((
            pos0 + distance + lanes,
            [
                jnp.where(distance + 8 * v >= exclusion, pos0 + distance + lanes, NOWHERE)
                if ahead
                else jnp.where(-8 * v - distance >= exclusion, pos0 + distance + lanes, -NOWHERE)
                for v in range(STEPS)
            ],
        ))
        scaled.append({})
        hankel(a_ref, row, lane, SCORE_BLOCKS, scaled[-1].__setitem__)
        shifted.append({})
        hankel(b_ref, row, lane, SCORE_BLOCKS, shifted[-1].__setitem__)

    for j in range(SCORE_BLOCKS):
        for v in range(STEPS):
            here, middle, after = at(j, v), at(j + 1, v), at(j + 2, v)
            mean = rows_of(own_mean, v, j)
            top = best[here, :]
            for i in range(len(sides)):
                sums = scratch[i][1]
                products = sums[here, :128] + (sums[middle, :128] + sums[middle, 128:]) + sums[after, 128:]
                score = products * scaled[i][j] - mean * shifted[i][j]
                partner = masks[i][1][v]
                counted = partner < total - 128 * j if sides[i][0] else partner >= -128 * j
                top = jnp.maximum(top, jnp.where(counted, score, -FILL))
            best[here, :] = top


def finish(best, a_ref, out_ref):
    def part(j, v):
        return best[(STEPS * j + v) * 8 : (STEPS * j + v) * 8 + 8, :]

    lanes = lax.broadcasted_iota(jnp.int32, (8, 128), 1)
    tops = [part(j, 0) for j in range(OWN)]
    for v in range(1, STEPS):
        moved = [pltpu.roll(part(j, v), 128 - 8 * v, 1) for j in range(SCORE_BLOCKS)]
        for j in range(OWN):
            tops[j] = jnp.maximum(tops[j], jnp.where(lanes < 128 - 8 * v, moved[j], moved[j + 1]))
    top = jnp.concatenate([jnp.max(t, axis=0, keepdims=True) for t in tops], axis=0)
    corr = top * (a_ref[HALO : HALO + OWN, :] * float(M))
    out_ref[...] = jnp.where(top < -0.1 * FILL, FILL, jnp.sqrt(1.0 - corr))


def kernel(
    series_hbm, tail_hbm, offset_hbm, exclusion_hbm, out,
    series, tail, offset, exclusion,
    ext, x_ref, mean_ref, a_ref, b_ref, w_ref, ones_ref,
    x_skew, a_skew, b_skew, own_x, own_mean,
    lhs0, sums0, lhs1, sums1, lhs2, sums2, lhs3, sums3, best,
    mine, gathered, load_sem, halo_send, halo_recv, off_send, off_recv,
    *, n_tm, n_diag, total,
):
    tm = lax.axis_index("tm")
    z = lax.axis_index("diag")
    has_prev = tm > 0
    has_next = tm < n_tm - 1

    def peer(h):
        return (tm, lax.rem(z + h + n_diag, n_diag))

    barrier = pltpu.get_barrier_semaphore()

    @pl.when(has_prev)
    def _():
        pl.semaphore_signal(barrier, inc=1, device_id=(tm - 1, z), device_id_type=MESH)

    @pl.when(has_next)
    def _():
        pl.semaphore_signal(barrier, inc=1, device_id=(tm + 1, z), device_id_type=MESH)

    for k in range(2 * NEAR, 0, -1):
        pl.semaphore_signal(barrier, inc=1, device_id=peer(hop(k)), device_id_type=MESH)

    loads = [
        pltpu.make_async_copy(source, target, load_sem.at[i])
        for i, (source, target) in enumerate(
            ((offset_hbm, offset), (series_hbm, series), (tail_hbm, tail), (exclusion_hbm, exclusion))
        )
    ]
    for load in loads:
        load.start()

    ext[2 * HALO + SEG :, :] = jnp.zeros((EXT - 2 * HALO - SEG, 128), F32)
    w_ref[...] = window_weights()
    ones_ref[...] = w_ref[...].astype(F32)
    scratch = ((lhs0, sums0), (lhs1, sums1), (lhs2, sums2), (lhs3, sums3))
    best[...] = jnp.full(best.shape, -FILL, F32)

    edge = has_prev.astype(jnp.int32) + has_next.astype(jnp.int32)
    for load in loads:
        load.wait()

    mine[0, 0] = offset[0]
    gathered[0, 0] = offset[0]
    ext[HALO : HALO + SEG, :] = series[...]

    @pl.when(jnp.logical_not(has_prev))
    def _():
        ext[:HALO, :] = jnp.zeros((HALO, 128), F32)

    @pl.when(jnp.logical_not(has_next))
    def _():
        ext[HALO + SEG : HALO + SEG + 2, :] = tail[...]
        ext[HALO + SEG + 2 : 2 * HALO + SEG, :] = jnp.zeros((HALO - 2, 128), F32)

    pl.semaphore_wait(barrier, 2 * NEAR + edge)

    def offset_copy(k):
        h = hop(k)
        near = abs(h) <= NEAR
        source = mine if near else gathered.at[pl.ds(k - 2 * NEAR, 1)]
        to = -h if near else (-NEAR if h > 0 else NEAR)
        return pltpu.make_async_remote_copy(
            source, gathered.at[pl.ds(k, 1)], off_send.at[k], off_recv.at[k],
            device_id=peer(to), device_id_type=MESH,
        )

    to_prev = pltpu.make_async_remote_copy(
        series.at[pl.ds(0, HALO)], ext.at[pl.ds(HALO + SEG, HALO)], halo_send.at[0], halo_recv.at[0],
        device_id=(tm - 1, z), device_id_type=MESH,
    )
    to_next = pltpu.make_async_remote_copy(
        series.at[pl.ds(SEG - HALO, HALO)], ext.at[pl.ds(0, HALO)], halo_send.at[1], halo_recv.at[1],
        device_id=(tm + 1, z), device_id_type=MESH,
    )

    for k in range(2 * NEAR, 0, -1):
        offset_copy(k).start()

    @pl.when(has_prev)
    def _():
        to_prev.start()

    @pl.when(has_next)
    def _():
        to_next.start()

    for k in range(1, 2 * NEAR + 1):
        offset_copy(k).wait_recv()
        if k + 2 * NEAR < n_diag:
            offset_copy(k + 2 * NEAR).start()

    @pl.when(has_next)
    def _():
        to_prev.wait_recv()

    @pl.when(has_prev)
    def _():
        to_next.wait_recv()

    x_ref[...] = ext[pl.ds(pl.multiple_of(OWN * z, OWN), REGION), :]
    window_stats(x_ref, w_ref, mean_ref, a_ref, b_ref)
    skewed(((x_ref, x_skew), (a_ref, a_skew), (b_ref, b_skew)))
    own_rows(x_ref, own_x)
    own_rows(mean_ref, own_mean)
    pos0 = (tm * SEG + z * OWN) * 128

    def pair(t, carry):
        for i in range(2):

            @pl.when(2 * t + i > 2 * NEAR)
            def _(k=2 * t + i):
                pltpu.make_async_remote_copy(
                    mine, gathered.at[pl.ds(k, 1)], off_send.at[k], off_recv.at[k],
                    device_id=peer(1), device_id_type=MESH,
                ).wait_recv()

        group_scores(
            (gathered[2 * t, 0], gathered[2 * t + 1, 0]), exclusion[0], pos0, total,
            x_skew, a_skew, b_skew, own_x, own_mean, ones_ref, scratch, best,
        )
        return carry

    lax.fori_loop(0, n_diag // 2, pair, 0)
    finish(best, a_ref, out)

    for k in range(1, n_diag):
        offset_copy(k).wait_send()

    @pl.when(has_prev)
    def _():
        to_prev.wait_send()

    @pl.when(has_next)
    def _():
        to_next.wait_send()


def solution(mesh):
    n_tm, n_diag = mesh.shape["tm"], mesh.shape["diag"]

    def on_device(series, tail, diag_offsets, exclusion):
        total = series.shape[0] * n_tm
        anywhere = pl.BlockSpec(memory_space=pltpu.HBM)
        product_rows = KB * (SCORE_BLOCKS + 2)
        side_scratch = [pltpu.VMEM((product_rows, 256), F32)] * 2
        rows = pl.pallas_call(
            functools.partial(kernel, n_tm=n_tm, n_diag=n_diag, total=total),
            out_shape=jax.ShapeDtypeStruct((OWN, 128), F32),
            in_specs=[anywhere] * 4,
            out_specs=pl.BlockSpec(memory_space=pltpu.VMEM),
            scratch_shapes=[
                pltpu.VMEM((SEG, 128), F32),
                pltpu.VMEM((M // 128, 128), F32),
                pltpu.SMEM((1,), jnp.int32),
                pltpu.SMEM((1,), jnp.int32),
                pltpu.VMEM((EXT, 128), F32),
                pltpu.VMEM((REGION, 128), F32),
                pltpu.VMEM((REGION, 128), F32),
                pltpu.VMEM((REGION, 128), F32),
                pltpu.VMEM((REGION, 128), F32),
                pltpu.VMEM((256, 256), BF16),
                pltpu.VMEM((256, 256), F32),
                pltpu.VMEM((8 * SKEWED, 128), F32),
                pltpu.VMEM((8 * SKEWED, 128), F32),
                pltpu.VMEM((8 * SKEWED, 128), F32),
                pltpu.VMEM((16 * STEPS, 128), F32),
                pltpu.VMEM((16 * STEPS, 128), F32),
                *side_scratch * 4,
                pltpu.VMEM((KB * SCORE_BLOCKS, 128), F32),
                pltpu.SMEM((1, 128), jnp.int32),
                pltpu.SMEM((16, 128), jnp.int32),
                pltpu.SemaphoreType.DMA((4,)),
                pltpu.SemaphoreType.DMA((2,)),
                pltpu.SemaphoreType.DMA((2,)),
                pltpu.SemaphoreType.DMA((16,)),
                pltpu.SemaphoreType.DMA((16,)),
            ],
            compiler_params=pltpu.CompilerParams(collective_id=0, has_side_effects=True),
            name="profile_rows",
        )(
            series.reshape(SEG, 128),
            tail.reshape(M // 128, 128),
            diag_offsets,
            exclusion,
        )
        return rows.reshape(-1)

    in_specs = (P("tm"), P(), P("diag"), P())
    out_specs = P(("tm", "diag"))
    return jax.shard_map(
        on_device, mesh=mesh, in_specs=in_specs, out_specs=out_specs, check_vma=False
    )
```

```python
import functools

import jax
import jax.numpy as jnp
from jax import lax
from jax.experimental import pallas as pl
from jax.experimental.pallas import tpu as pltpu
from jax.sharding import PartitionSpec as P

F32 = jnp.float32
BF16 = jnp.bfloat16
MESH = pl.DeviceIdType.MESH

M = 256
KB = 32
LANES = 128
FILL = 1e30
NOWHERE = 1 << 30

HALO = 96
SEG = 128
OWN = 8
REGION = 2 * HALO + OWN + 16
SKEWED = REGION - 8
EXT = 2 * HALO + SEG + 16
STEPS = KB // 8
SCORE_BLOCKS = OWN + 1

HUBS = 4
SERVES = ((), (10, 11, 12, 13, 14, 15), (6, 7), (4, 5, 8, 9))


def split2(v):
    high = v.astype(BF16)
    return high, (v - high.astype(F32)).astype(BF16)


def window_weights():
    r = lax.broadcasted_iota(jnp.int32, (256, 256), 0) & 127
    c = lax.broadcasted_iota(jnp.int32, (256, 256), 1)
    from_c = jnp.where(r >= c, 1.0, 0.0)
    before_c = jnp.where(r < c - 128, 1.0, 0.0)
    return jnp.where(c < 128, from_c, before_c).astype(BF16)


def window_stats(x_ref, w_ref, mean_ref, a_ref, b_ref):
    def window_sums(v):
        high, mid = split2(v)
        low = (v - high.astype(F32) - mid.astype(F32)).astype(BF16)
        g = jnp.dot(jnp.concatenate([high, mid], axis=1), w_ref[...], preferred_element_type=F32)
        g = g + jnp.dot(low, w_ref[:128, :], preferred_element_type=F32)
        from_c, before_c = g[:, :128], g[:, 128:]
        n = v.shape[0]
        return from_c[: n - 2] + (from_c + before_c)[1 : n - 1] + before_c[2:]

    x = x_ref[...]
    n = x.shape[0] - 2
    first = window_sums(x) * (1.0 / M)
    second = window_sums(x * x) * (1.0 / M)
    spread = 1.0 / jnp.sqrt(second - first * first + 1e-5)
    mean_ref[:n, :] = first
    a_ref[:n, :] = spread * (1.0 / M)
    b_ref[:n, :] = first * spread


def own_rows(ref, out_ref):
    n = 16
    here = ref[HALO : HALO + n, :]
    before = ref[HALO - 1 : HALO - 1 + n, :]
    lanes = lax.broadcasted_iota(jnp.int32, (n, 128), 1)
    out_ref[:n, :] = here
    for v in range(1, STEPS):
        shift = 8 * v
        out_ref[n * v : n * v + n, :] = jnp.where(
            lanes < shift, pltpu.roll(before, shift, 1), pltpu.roll(here, shift, 1)
        )


def skewed(pairs):
    lanes = lax.broadcasted_iota(jnp.int32, (8, 128), 1)
    subs = lax.broadcasted_iota(jnp.int32, (8, 128), 0)
    here = lanes < 121 + subs
    batch = SKEWED // 4

    def rows(i, carry):
        start = batch * i
        for ref, out_ref in pairs:
            last = None
            for j in range(batch + 1):
                row = jnp.broadcast_to(ref[pl.ds(start + j, 1), :], (8, 128))
                rolled = pltpu.roll(row, 121, 1, stride=1, stride_axis=0)
                if j:
                    out_ref[pl.ds(pl.multiple_of(8 * (start + j - 1), 8), 8), :] = jnp.where(here, last, rolled)
                last = rolled
        return carry

    lax.fori_loop(0, SKEWED // batch, rows, 0)


def hankel(ref, row, lane, blocks, emit):
    lanes = lax.broadcasted_iota(jnp.int32, (8, 128), 1)
    here = lanes < 128 - lane
    shift = (128 - lane) & 127
    rolled = [
        pltpu.roll(ref[pl.ds(8 * row + 8 * j, 8), :], shift, 1) for j in range(blocks + 1)
    ]
    for j in range(blocks):
        emit(j, jnp.where(here, rolled[j], rolled[j + 1]))


def group_scores(
    firsts, exclusion, pos0, total, x_ref, a_ref, b_ref, own_x, own_mean, w_ref, scratch, best
):
    subs = lax.broadcasted_iota(jnp.int32, (8, 128), 0)
    lanes = lax.broadcasted_iota(jnp.int32, (8, 128), 1)

    def rows_of(ref, v, j):
        return jnp.broadcast_to(ref[16 * v + j : 16 * v + j + 1, :], (8, 128))

    def at(j, v):
        return slice((STEPS * j + v) * 8, (STEPS * j + v) * 8 + 8)

    sides = []
    for first in firsts:
        for ahead in (True, False):
            beta = first if ahead else -first - (KB - 1)
            start = HALO * 128 + beta
            sides.append((ahead, beta, lax.shift_right_arithmetic(start, 7), start & 127))

    for (_, _, row, lane), (lhs, _) in zip(sides, scratch):

        def emit_products(j, y, lhs=lhs):
            own = jnp.concatenate([rows_of(own_x, v, j) for v in range(STEPS)], axis=0)
            p = jnp.concatenate([y] * STEPS, axis=0) * own
            lhs[KB * j : KB * j + KB, :128] = p
            lhs[KB * j : KB * j + KB, 128:] = p - p.astype(BF16).astype(F32)

        hankel(x_ref, row, lane, SCORE_BLOCKS + 2, emit_products)

    for lhs, sums in scratch[: len(sides)]:
        sums[...] = jnp.dot(lhs[...], w_ref[...], preferred_element_type=F32)

    masks, scaled, shifted = [], [], []
    for ahead, beta, row, lane in sides:
        distance = beta + 7 - subs
        masks.append((
            pos0 + distance + lanes,
            [
                jnp.where(distance + 8 * v >= exclusion, pos0 + distance + lanes, NOWHERE)
                if ahead
                else jnp.where(-8 * v - distance >= exclusion, pos0 + distance + lanes, -NOWHERE)
                for v in range(STEPS)
            ],
        ))
        scaled.append({})
        hankel(a_ref, row, lane, SCORE_BLOCKS, scaled[-1].__setitem__)
        shifted.append({})
        hankel(b_ref, row, lane, SCORE_BLOCKS, shifted[-1].__setitem__)

    for j in range(SCORE_BLOCKS):
        for v in range(STEPS):
            here, middle, after = at(j, v), at(j + 1, v), at(j + 2, v)
            mean = rows_of(own_mean, v, j)
            top = best[here, :]
            for i in range(len(sides)):
                sums = scratch[i][1]
                products = sums[here, :128] + (sums[middle, :128] + sums[middle, 128:]) + sums[after, 128:]
                score = products * scaled[i][j] - mean * shifted[i][j]
                partner = masks[i][1][v]
                counted = partner < total - 128 * j if sides[i][0] else partner >= -128 * j
                top = jnp.maximum(top, jnp.where(counted, score, -FILL))
            best[here, :] = top


def finish(best, a_ref, out_ref):
    def part(j, v):
        return best[(STEPS * j + v) * 8 : (STEPS * j + v) * 8 + 8, :]

    lanes = lax.broadcasted_iota(jnp.int32, (8, 128), 1)
    tops = [part(j, 0) for j in range(OWN)]
    for v in range(1, STEPS):
        moved = [pltpu.roll(part(j, v), 128 - 8 * v, 1) for j in range(SCORE_BLOCKS)]
        for j in range(OWN):
            tops[j] = jnp.maximum(tops[j], jnp.where(lanes < 128 - 8 * v, moved[j], moved[j + 1]))
    top = jnp.concatenate([jnp.max(t, axis=0, keepdims=True) for t in tops], axis=0)
    corr = top * (a_ref[HALO : HALO + OWN, :] * float(M))
    out_ref[...] = jnp.where(top < -0.1 * FILL, FILL, jnp.sqrt(1.0 - corr))


def kernel(
    series_hbm, tail_hbm, offset, exclusion, out,
    series, tail,
    ext, x_ref, mean_ref, a_ref, b_ref, w_ref, ones_ref,
    x_skew, a_skew, b_skew, own_x, own_mean,
    lhs0, sums0, lhs1, sums1, lhs2, sums2, lhs3, sums3, best,
    mine, table, packed, load_sem, halo_send, halo_recv, row_send, row_recv, reply_send, table_send, table_recv, answer,
    *, n_tm, n_diag, total,
):
    tm = lax.axis_index("tm")
    z = lax.axis_index("diag")
    has_prev = tm > 0
    has_next = tm < n_tm - 1

    is_hub = z < HUBS

    barrier = pltpu.get_barrier_semaphore()

    answers = lax.rem(tm, 2) == 1

    @pl.when(jnp.logical_not(answers) & has_prev)
    def _():
        pl.semaphore_signal(barrier, inc=1, device_id=(tm - 1, z), device_id_type=MESH)

    @pl.when(jnp.logical_not(answers) & has_next)
    def _():
        pl.semaphore_signal(barrier, inc=1, device_id=(tm + 1, z), device_id_type=MESH)

    for b in range(n_diag - 1, 0, -1):

        @pl.when(is_hub & (z < b))
        def _(b=b):
            pl.semaphore_signal(barrier, inc=1, device_id=(tm, b), device_id_type=MESH)

    mine[0, 0] = offset[0]

    @pl.when(is_hub)
    def _():
        table[z, 0] = offset[0]

    loads = [
        pltpu.make_async_copy(source, target, load_sem.at[i])
        for i, (source, target) in enumerate(
            ((series_hbm, series), (tail_hbm, tail))
        )
    ]
    for load in loads:
        load.start()

    def row_copy(to, send_sem):
        return pltpu.make_async_remote_copy(
            mine, table.at[pl.ds(z, 1)], send_sem, row_recv.at[z], device_id=(tm, to), device_id_type=MESH
        )

    def wait_row(b):
        pltpu.make_async_remote_copy(
            mine, table.at[pl.ds(b, 1)], row_send.at[0], row_recv.at[b], device_id=(tm, 0), device_id_type=MESH
        ).wait_recv()

    half = n_diag // 2

    def table_copy(to, i, part):
        rows = packed.at[pl.ds(part, 1)]
        return pltpu.make_async_remote_copy(
            rows, rows, table_send.at[2 * i + part], table_recv.at[part], device_id=(tm, to), device_id_type=MESH
        )

    to_prev = pltpu.make_async_remote_copy(
        series.at[pl.ds(0, HALO)], ext.at[pl.ds(HALO + SEG, HALO)], halo_send.at[0], halo_recv.at[0],
        device_id=(tm - 1, z), device_id_type=MESH,
    )
    to_next = pltpu.make_async_remote_copy(
        series.at[pl.ds(SEG - HALO, HALO)], ext.at[pl.ds(0, HALO)], halo_send.at[1], halo_recv.at[1],
        device_id=(tm + 1, z), device_id_type=MESH,
    )

    edge = has_prev.astype(jnp.int32) + has_next.astype(jnp.int32)
    announced = jnp.minimum(z, HUBS) + edge * lax.rem(tm, 2)

    @pl.when(announced > 0)
    def _():
        pl.semaphore_wait(barrier, announced)

    @pl.when(answers & has_prev)
    def _():
        pl.semaphore_signal(answer.at[1], inc=1, device_id=(tm - 1, z), device_id_type=MESH)

    @pl.when(answers & has_next)
    def _():
        pl.semaphore_signal(answer.at[0], inc=1, device_id=(tm + 1, z), device_id_type=MESH)

    for a in range(HUBS):

        @pl.when(z > a)
        def _(a=a):
            row_copy(a, row_send.at[a]).start()

    for load in loads:
        load.wait()

    @pl.when(has_prev)
    def _():
        @pl.when(jnp.logical_not(answers))
        def _():
            pl.semaphore_wait(answer.at[0], 1)

        to_prev.start()

    @pl.when(has_next)
    def _():
        @pl.when(jnp.logical_not(answers))
        def _():
            pl.semaphore_wait(answer.at[1], 1)

        to_next.start()

    ext[HALO : HALO + SEG, :] = series[...]
    ext[2 * HALO + SEG :, :] = jnp.zeros((EXT - 2 * HALO - SEG, 128), F32)

    @pl.when(jnp.logical_not(has_prev))
    def _():
        ext[:HALO, :] = jnp.zeros((HALO, 128), F32)

    @pl.when(jnp.logical_not(has_next))
    def _():
        ext[HALO + SEG : HALO + SEG + 2, :] = tail[...]
        ext[HALO + SEG + 2 : 2 * HALO + SEG, :] = jnp.zeros((HALO - 2, 128), F32)

    w_ref[...] = window_weights()
    ones_ref[...] = w_ref[...].astype(F32)
    scratch = ((lhs0, sums0), (lhs1, sums1), (lhs2, sums2), (lhs3, sums3))
    best[...] = jnp.full(best.shape, -FILL, F32)

    @pl.when(has_next)
    def _():
        to_prev.wait_recv()

    @pl.when(has_prev)
    def _():
        to_next.wait_recv()

    x_ref[...] = ext[pl.ds(pl.multiple_of(OWN * z, OWN), REGION), :]
    window_stats(x_ref, w_ref, mean_ref, a_ref, b_ref)
    skewed(((x_ref, x_skew), (a_ref, a_skew), (b_ref, b_skew)))
    own_rows(x_ref, own_x)
    own_rows(mean_ref, own_mean)
    pos0 = (tm * SEG + z * OWN) * 128

    for b in range(1, HUBS):

        @pl.when(z < b)
        def _(b=b):
            wait_row(b)
            row_copy(b, reply_send.at[b]).start()

    for a in range(HUBS - 1):

        @pl.when(is_hub & (z > a))
        def _(a=a):
            wait_row(a)

    @pl.when(is_hub)
    def _():
        for b in range(HUBS, half):
            wait_row(b)

        for b in range(half):
            packed[0, b] = table[b, 0]

    for hub, served in enumerate(SERVES):

        @pl.when(z == hub)
        def _(served=served):
            for i, to in enumerate(served):
                if to < half:
                    table_copy(to, i, 0).start()

    @pl.when(jnp.logical_not(is_hub))
    def _():
        table_copy(0, 0, 0).wait_recv()

    def pair(t, carry):
        @pl.when(jnp.logical_not(is_hub) & (t == half // 2))
        def _():
            table_copy(0, 0, 1).wait_recv()

        @pl.when(is_hub & (t == half // 2))
        def _():
            for b in range(half, n_diag):
                wait_row(b)
                packed[1, b - half] = table[b, 0]
            for hub, served in enumerate(SERVES):

                @pl.when(z == hub)
                def _(served=served):
                    for i, to in enumerate(served):
                        if to >= half:
                            table_copy(to, i, 0).start()
                        table_copy(to, i, 1).start()

        part = jnp.where(t < half // 2, 0, 1)
        column = 2 * t - half * part
        group_scores(
            (packed[part, column], packed[part, column + 1]), exclusion[0], pos0, total,
            x_skew, a_skew, b_skew, own_x, own_mean, ones_ref, scratch, best,
        )
        return carry

    lax.fori_loop(0, n_diag // 2, pair, 0)
    finish(best, a_ref, out)

    for a in range(HUBS):

        @pl.when(z > a)
        def _(a=a):
            row_copy(a, row_send.at[a]).wait_send()

    for b in range(1, HUBS):

        @pl.when(z < b)
        def _(b=b):
            row_copy(b, reply_send.at[b]).wait_send()

    for hub, served in enumerate(SERVES):

        @pl.when(z == hub)
        def _(served=served):
            for i, to in enumerate(served):
                table_copy(to, i, 0).wait_send()
                table_copy(to, i, 1).wait_send()

    @pl.when(has_prev)
    def _():
        to_prev.wait_send()

    @pl.when(has_next)
    def _():
        to_next.wait_send()


def solution(mesh):
    n_tm, n_diag = mesh.shape["tm"], mesh.shape["diag"]

    def on_device(series, tail, diag_offsets, exclusion):
        total = series.shape[0] * n_tm
        anywhere = pl.BlockSpec(memory_space=pl.ANY)
        smem = pl.BlockSpec(memory_space=pltpu.SMEM)
        product_rows = KB * (SCORE_BLOCKS + 2)
        side_scratch = [pltpu.VMEM((product_rows, 256), F32)] * 2
        rows = pl.pallas_call(
            functools.partial(kernel, n_tm=n_tm, n_diag=n_diag, total=total),
            out_shape=jax.ShapeDtypeStruct((OWN, 128), F32),
            in_specs=[anywhere, anywhere, smem, smem],
            out_specs=pl.BlockSpec(memory_space=pltpu.VMEM),
            scratch_shapes=[
                pltpu.VMEM((SEG, 128), F32),
                pltpu.VMEM((M // 128, 128), F32),
                pltpu.VMEM((EXT, 128), F32),
                pltpu.VMEM((REGION, 128), F32),
                pltpu.VMEM((REGION, 128), F32),
                pltpu.VMEM((REGION, 128), F32),
                pltpu.VMEM((REGION, 128), F32),
                pltpu.VMEM((256, 256), BF16),
                pltpu.VMEM((256, 256), F32),
                pltpu.VMEM((8 * SKEWED, 128), F32),
                pltpu.VMEM((8 * SKEWED, 128), F32),
                pltpu.VMEM((8 * SKEWED, 128), F32),
                pltpu.VMEM((16 * STEPS, 128), F32),
                pltpu.VMEM((16 * STEPS, 128), F32),
                *side_scratch * 4,
                pltpu.VMEM((KB * SCORE_BLOCKS, 128), F32),
                pltpu.SMEM((1, 128), jnp.int32),
                pltpu.SMEM((16, 128), jnp.int32),
                pltpu.SMEM((2, 128), jnp.int32),
                pltpu.SemaphoreType.DMA((2,)),
                pltpu.SemaphoreType.DMA((2,)),
                pltpu.SemaphoreType.DMA((2,)),
                pltpu.SemaphoreType.DMA((HUBS,)),
                pltpu.SemaphoreType.DMA((16,)),
                pltpu.SemaphoreType.DMA((HUBS,)),
                pltpu.SemaphoreType.DMA((2 * max(map(len, SERVES)),)),
                pltpu.SemaphoreType.DMA((2,)),
                pltpu.SemaphoreType.REGULAR((2,)),
            ],
            compiler_params=pltpu.CompilerParams(collective_id=0, has_side_effects=True),
            name="profile_rows",
        )(
            series.reshape(SEG, 128),
            tail.reshape(M // 128, 128),
            diag_offsets,
            exclusion,
        )
        return rows.reshape(-1)

    in_specs = (P("tm"), P(), P("diag"), P())
    out_specs = P(("tm", "diag"))
    return jax.shard_map(
        on_device, mesh=mesh, in_specs=in_specs, out_specs=out_specs, check_vma=False
    )
```

```python
import functools

import jax
import jax.numpy as jnp
from jax import lax
from jax.experimental import pallas as pl
from jax.experimental.pallas import tpu as pltpu
from jax.sharding import PartitionSpec as P

F32 = jnp.float32
BF16 = jnp.bfloat16
MESH = pl.DeviceIdType.MESH

M = 256
KB = 32
LANES = 128
FILL = 1e30
NOWHERE = 1 << 30

HALO = 96
SEG = 128
OWN = 8
REGION = 2 * HALO + OWN + 16
SKEWED = REGION - 8
EXT = 2 * HALO + SEG + 16
STEPS = KB // 8
SCORE_BLOCKS = OWN + 1

HUBS = 4
SERVES = ((), (0, 10, 11, 12, 13, 14, 15), (6, 7), (4, 5, 8, 9))


def split2(v):
    high = v.astype(BF16)
    return high, (v - high.astype(F32)).astype(BF16)


def window_weights():
    r = lax.broadcasted_iota(jnp.int32, (256, 256), 0) & 127
    c = lax.broadcasted_iota(jnp.int32, (256, 256), 1)
    from_c = jnp.where(r >= c, 1.0, 0.0)
    before_c = jnp.where(r < c - 128, 1.0, 0.0)
    return jnp.where(c < 128, from_c, before_c).astype(BF16)


def window_stats(x_ref, w_ref, mean_ref, a_ref, b_ref):
    def window_sums(v):
        high, mid = split2(v)
        low = (v - high.astype(F32) - mid.astype(F32)).astype(BF16)
        g = jnp.dot(jnp.concatenate([high, mid], axis=1), w_ref[...], preferred_element_type=F32)
        g = g + jnp.dot(low, w_ref[:128, :], preferred_element_type=F32)
        from_c, before_c = g[:, :128], g[:, 128:]
        n = v.shape[0]
        return from_c[: n - 2] + (from_c + before_c)[1 : n - 1] + before_c[2:]

    x = x_ref[...]
    n = x.shape[0] - 2
    first = window_sums(x) * (1.0 / M)
    second = window_sums(x * x) * (1.0 / M)
    spread = 1.0 / jnp.sqrt(second - first * first + 1e-5)
    mean_ref[:n, :] = first
    a_ref[:n, :] = spread * (1.0 / M)
    b_ref[:n, :] = first * spread


def own_rows(ref, out_ref):
    n = 16
    here = ref[HALO : HALO + n, :]
    before = ref[HALO - 1 : HALO - 1 + n, :]
    lanes = lax.broadcasted_iota(jnp.int32, (n, 128), 1)
    out_ref[:n, :] = here
    for v in range(1, STEPS):
        shift = 8 * v
        out_ref[n * v : n * v + n, :] = jnp.where(
            lanes < shift, pltpu.roll(before, shift, 1), pltpu.roll(here, shift, 1)
        )


def skewed(pairs):
    lanes = lax.broadcasted_iota(jnp.int32, (8, 128), 1)
    subs = lax.broadcasted_iota(jnp.int32, (8, 128), 0)
    here = lanes < 121 + subs
    batch = SKEWED // 4

    def rows(i, carry):
        start = batch * i
        for ref, out_ref in pairs:
            last = None
            for j in range(batch + 1):
                row = jnp.broadcast_to(ref[pl.ds(start + j, 1), :], (8, 128))
                rolled = pltpu.roll(row, 121, 1, stride=1, stride_axis=0)
                if j:
                    out_ref[pl.ds(pl.multiple_of(8 * (start + j - 1), 8), 8), :] = jnp.where(here, last, rolled)
                last = rolled
        return carry

    lax.fori_loop(0, SKEWED // batch, rows, 0)


def hankel(ref, row, lane, blocks, emit):
    lanes = lax.broadcasted_iota(jnp.int32, (8, 128), 1)
    here = lanes < 128 - lane
    shift = (128 - lane) & 127
    rolled = [
        pltpu.roll(ref[pl.ds(8 * row + 8 * j, 8), :], shift, 1) for j in range(blocks + 1)
    ]
    for j in range(blocks):
        emit(j, jnp.where(here, rolled[j], rolled[j + 1]))


def group_scores(
    firsts, exclusion, pos0, total, x_ref, a_ref, b_ref, own_x, own_mean, w_ref, scratch, best
):
    subs = lax.broadcasted_iota(jnp.int32, (8, 128), 0)
    lanes = lax.broadcasted_iota(jnp.int32, (8, 128), 1)

    def rows_of(ref, v, j):
        return jnp.broadcast_to(ref[16 * v + j : 16 * v + j + 1, :], (8, 128))

    def at(j, v):
        return slice((STEPS * j + v) * 8, (STEPS * j + v) * 8 + 8)

    sides = []
    for first in firsts:
        for ahead in (True, False):
            beta = first if ahead else -first - (KB - 1)
            start = HALO * 128 + beta
            sides.append((ahead, beta, lax.shift_right_arithmetic(start, 7), start & 127))

    for (_, _, row, lane), (lhs, _) in zip(sides, scratch):

        def emit_products(j, y, lhs=lhs):
            own = jnp.concatenate([rows_of(own_x, v, j) for v in range(STEPS)], axis=0)
            p = jnp.concatenate([y] * STEPS, axis=0) * own
            lhs[KB * j : KB * j + KB, :128] = p
            lhs[KB * j : KB * j + KB, 128:] = p - p.astype(BF16).astype(F32)

        hankel(x_ref, row, lane, SCORE_BLOCKS + 2, emit_products)

    for lhs, sums in scratch[: len(sides)]:
        sums[...] = jnp.dot(lhs[...], w_ref[...], preferred_element_type=F32)

    masks, scaled, shifted = [], [], []
    for ahead, beta, row, lane in sides:
        distance = beta + 7 - subs
        masks.append((
            pos0 + distance + lanes,
            [
                jnp.where(distance + 8 * v >= exclusion, pos0 + distance + lanes, NOWHERE)
                if ahead
                else jnp.where(-8 * v - distance >= exclusion, pos0 + distance + lanes, -NOWHERE)
                for v in range(STEPS)
            ],
        ))
        scaled.append({})
        hankel(a_ref, row, lane, SCORE_BLOCKS, scaled[-1].__setitem__)
        shifted.append({})
        hankel(b_ref, row, lane, SCORE_BLOCKS, shifted[-1].__setitem__)

    for j in range(SCORE_BLOCKS):
        for v in range(STEPS):
            here, middle, after = at(j, v), at(j + 1, v), at(j + 2, v)
            mean = rows_of(own_mean, v, j)
            top = best[here, :]
            for i in range(len(sides)):
                sums = scratch[i][1]
                products = sums[here, :128] + (sums[middle, :128] + sums[middle, 128:]) + sums[after, 128:]
                score = products * scaled[i][j] - mean * shifted[i][j]
                partner = masks[i][1][v]
                counted = partner < total - 128 * j if sides[i][0] else partner >= -128 * j
                top = jnp.maximum(top, jnp.where(counted, score, -FILL))
            best[here, :] = top


def finish(best, a_ref, out_ref):
    def part(j, v):
        return best[(STEPS * j + v) * 8 : (STEPS * j + v) * 8 + 8, :]

    lanes = lax.broadcasted_iota(jnp.int32, (8, 128), 1)
    tops = [part(j, 0) for j in range(OWN)]
    for v in range(1, STEPS):
        moved = [pltpu.roll(part(j, v), 128 - 8 * v, 1) for j in range(SCORE_BLOCKS)]
        for j in range(OWN):
            tops[j] = jnp.maximum(tops[j], jnp.where(lanes < 128 - 8 * v, moved[j], moved[j + 1]))
    top = jnp.concatenate([jnp.max(t, axis=0, keepdims=True) for t in tops], axis=0)
    corr = top * (a_ref[HALO : HALO + OWN, :] * float(M))
    out_ref[...] = jnp.where(top < -0.1 * FILL, FILL, jnp.sqrt(1.0 - corr))


def kernel(
    series_hbm, tail_hbm, offset, exclusion, out,
    series, tail,
    ext, x_ref, mean_ref, a_ref, b_ref, w_ref, ones_ref,
    x_skew, a_skew, b_skew, own_x, own_mean,
    lhs0, sums0, lhs1, sums1, lhs2, sums2, lhs3, sums3, best,
    mine, table, packed, load_sem, halo_send, halo_recv, row_send, row_recv, reply_send, table_send, table_recv, answer,
    *, n_tm, n_diag, total,
):
    tm = lax.axis_index("tm")
    z = lax.axis_index("diag")
    has_prev = tm > 0
    has_next = tm < n_tm - 1

    late = tm == 0
    is_hub = (z < HUBS) & jnp.logical_not(late & (z == 0))
    served_zero = late & (z == 0)

    barrier = pltpu.get_barrier_semaphore()

    answers = lax.rem(tm, 2) == 1

    @pl.when(jnp.logical_not(answers) & has_prev)
    def _():
        pl.semaphore_signal(barrier, inc=1, device_id=(tm - 1, z), device_id_type=MESH)

    @pl.when(jnp.logical_not(answers) & has_next)
    def _():
        pl.semaphore_signal(barrier, inc=1, device_id=(tm + 1, z), device_id_type=MESH)

    for b in range(n_diag - 1, 0, -1):

        @pl.when(is_hub & (z < b))
        def _(b=b):
            pl.semaphore_signal(barrier, inc=1, device_id=(tm, b), device_id_type=MESH)

    @pl.when(is_hub & late)
    def _():
        pl.semaphore_signal(barrier, inc=1, device_id=(tm, 0), device_id_type=MESH)

    mine[0, 0] = offset[0]

    @pl.when(is_hub)
    def _():
        table[z, 0] = offset[0]

    loads = [
        pltpu.make_async_copy(source, target, load_sem.at[i])
        for i, (source, target) in enumerate(
            ((series_hbm, series), (tail_hbm, tail))
        )
    ]
    for load in loads:
        load.start()

    def row_copy(to, send_sem):
        return pltpu.make_async_remote_copy(
            mine, table.at[pl.ds(z, 1)], send_sem, row_recv.at[z], device_id=(tm, to), device_id_type=MESH
        )

    def wait_row(b):
        pltpu.make_async_remote_copy(
            mine, table.at[pl.ds(b, 1)], row_send.at[0], row_recv.at[b], device_id=(tm, 0), device_id_type=MESH
        ).wait_recv()

    def sends_to(a):
        return (z > a) & jnp.logical_not(late) if a == 0 else (z > a) | served_zero

    half = n_diag // 2

    def table_copy(to, i, part):
        rows = packed.at[pl.ds(part, 1)]
        return pltpu.make_async_remote_copy(
            rows, rows, table_send.at[2 * i + part], table_recv.at[part], device_id=(tm, to), device_id_type=MESH
        )

    to_prev = pltpu.make_async_remote_copy(
        series.at[pl.ds(0, HALO)], ext.at[pl.ds(HALO + SEG, HALO)], halo_send.at[0], halo_recv.at[0],
        device_id=(tm - 1, z), device_id_type=MESH,
    )
    to_next = pltpu.make_async_remote_copy(
        series.at[pl.ds(SEG - HALO, HALO)], ext.at[pl.ds(0, HALO)], halo_send.at[1], halo_recv.at[1],
        device_id=(tm + 1, z), device_id_type=MESH,
    )

    edge = has_prev.astype(jnp.int32) + has_next.astype(jnp.int32)
    hubs_below = jnp.where(served_zero, HUBS - 1, jnp.minimum(z, HUBS) - (late & (z > 0)).astype(jnp.int32))
    announced = hubs_below + edge * lax.rem(tm, 2)

    @pl.when(announced > 0)
    def _():
        pl.semaphore_wait(barrier, announced)

    @pl.when(answers & has_prev)
    def _():
        pl.semaphore_signal(answer.at[1], inc=1, device_id=(tm - 1, z), device_id_type=MESH)

    @pl.when(answers & has_next)
    def _():
        pl.semaphore_signal(answer.at[0], inc=1, device_id=(tm + 1, z), device_id_type=MESH)

    for a in range(HUBS):

        @pl.when(sends_to(a))
        def _(a=a):
            row_copy(a, row_send.at[a]).start()

    for load in loads:
        load.wait()

    @pl.when(has_prev)
    def _():
        @pl.when(jnp.logical_not(answers))
        def _():
            pl.semaphore_wait(answer.at[0], 1)

        to_prev.start()

    @pl.when(has_next)
    def _():
        @pl.when(jnp.logical_not(answers))
        def _():
            pl.semaphore_wait(answer.at[1], 1)

        to_next.start()

    ext[HALO : HALO + SEG, :] = series[...]
    ext[2 * HALO + SEG :, :] = jnp.zeros((EXT - 2 * HALO - SEG, 128), F32)

    @pl.when(jnp.logical_not(has_prev))
    def _():
        ext[:HALO, :] = jnp.zeros((HALO, 128), F32)

    @pl.when(jnp.logical_not(has_next))
    def _():
        ext[HALO + SEG : HALO + SEG + 2, :] = tail[...]
        ext[HALO + SEG + 2 : 2 * HALO + SEG, :] = jnp.zeros((HALO - 2, 128), F32)

    w_ref[...] = window_weights()
    ones_ref[...] = w_ref[...].astype(F32)
    scratch = ((lhs0, sums0), (lhs1, sums1), (lhs2, sums2), (lhs3, sums3))
    best[...] = jnp.full(best.shape, -FILL, F32)

    @pl.when(has_next)
    def _():
        to_prev.wait_recv()

    @pl.when(has_prev)
    def _():
        to_next.wait_recv()

    x_ref[...] = ext[pl.ds(pl.multiple_of(OWN * z, OWN), REGION), :]
    window_stats(x_ref, w_ref, mean_ref, a_ref, b_ref)
    skewed(((x_ref, x_skew), (a_ref, a_skew), (b_ref, b_skew)))
    own_rows(x_ref, own_x)
    own_rows(mean_ref, own_mean)
    pos0 = (tm * SEG + z * OWN) * 128

    for b in range(1, HUBS):

        @pl.when(is_hub & (z < b))
        def _(b=b):
            wait_row(b)
            row_copy(b, reply_send.at[b]).start()

    for a in range(HUBS - 1):

        @pl.when(is_hub & (z > a))
        def _(a=a):
            wait_row(a)

    @pl.when(is_hub)
    def _():
        for b in range(HUBS, half):
            wait_row(b)

        for b in range(half):
            packed[0, b] = table[b, 0]

    for hub, served in enumerate(SERVES):

        @pl.when(z == hub)
        def _(served=served):
            for i, to in enumerate(served):
                if to < half:

                    @pl.when(late | (to > 0))
                    def _(i=i, to=to):
                        table_copy(to, i, 0).start()

    @pl.when(jnp.logical_not(is_hub))
    def _():
        table_copy(0, 0, 0).wait_recv()

    def pair(t, carry):
        @pl.when(jnp.logical_not(is_hub) & (t == half // 2))
        def _():
            table_copy(0, 0, 1).wait_recv()

        def take_row(b):
            wait_row(b)
            packed[1, b - half] = table[b, 0]

        for hub, served in enumerate(SERVES):
            if not served:
                for q in range(half // 2):

                    @pl.when(is_hub & (z == hub) & (t == half // 2 + q))
                    def _(q=q):
                        take_row(n_diag - 1 - 2 * q)
                        take_row(n_diag - 2 - 2 * q)

                continue

            @pl.when((z == hub) & (t == half // 2))
            def _(served=served):
                for i, to in enumerate(served):
                    if to >= half:
                        take_row(to)
                        table_copy(to, i, 0).start()
                for b in range(half, n_diag):
                    if b not in served:
                        take_row(b)
                for i, to in enumerate(served):

                    @pl.when(late | (to > 0))
                    def _(i=i, to=to):
                        table_copy(to, i, 1).start()

        part = jnp.where(t < half // 2, 0, 1)
        column = jnp.where(t < half // 2, 2 * t, 2 * (n_diag - half // 2 - 1 - t - half // 2))
        group_scores(
            (packed[part, column], packed[part, column + 1]), exclusion[0], pos0, total,
            x_skew, a_skew, b_skew, own_x, own_mean, ones_ref, scratch, best,
        )
        return carry

    lax.fori_loop(0, n_diag // 2, pair, 0)
    finish(best, a_ref, out)

    for a in range(HUBS):

        @pl.when(sends_to(a))
        def _(a=a):
            row_copy(a, row_send.at[a]).wait_send()

    for b in range(1, HUBS):

        @pl.when(is_hub & (z < b))
        def _(b=b):
            row_copy(b, reply_send.at[b]).wait_send()

    for hub, served in enumerate(SERVES):

        @pl.when(z == hub)
        def _(served=served):
            for i, to in enumerate(served):

                @pl.when(late | (to > 0))
                def _(i=i, to=to):
                    table_copy(to, i, 0).wait_send()
                    table_copy(to, i, 1).wait_send()

    @pl.when(has_prev)
    def _():
        to_prev.wait_send()

    @pl.when(has_next)
    def _():
        to_next.wait_send()


def solution(mesh):
    n_tm, n_diag = mesh.shape["tm"], mesh.shape["diag"]

    def on_device(series, tail, diag_offsets, exclusion):
        total = series.shape[0] * n_tm
        anywhere = pl.BlockSpec(memory_space=pl.ANY)
        smem = pl.BlockSpec(memory_space=pltpu.SMEM)
        product_rows = KB * (SCORE_BLOCKS + 2)
        side_scratch = [pltpu.VMEM((product_rows, 256), F32)] * 2
        rows = pl.pallas_call(
            functools.partial(kernel, n_tm=n_tm, n_diag=n_diag, total=total),
            out_shape=jax.ShapeDtypeStruct((OWN, 128), F32),
            in_specs=[anywhere, anywhere, smem, smem],
            out_specs=pl.BlockSpec(memory_space=pltpu.VMEM),
            scratch_shapes=[
                pltpu.VMEM((SEG, 128), F32),
                pltpu.VMEM((M // 128, 128), F32),
                pltpu.VMEM((EXT, 128), F32),
                pltpu.VMEM((REGION, 128), F32),
                pltpu.VMEM((REGION, 128), F32),
                pltpu.VMEM((REGION, 128), F32),
                pltpu.VMEM((REGION, 128), F32),
                pltpu.VMEM((256, 256), BF16),
                pltpu.VMEM((256, 256), F32),
                pltpu.VMEM((8 * SKEWED, 128), F32),
                pltpu.VMEM((8 * SKEWED, 128), F32),
                pltpu.VMEM((8 * SKEWED, 128), F32),
                pltpu.VMEM((16 * STEPS, 128), F32),
                pltpu.VMEM((16 * STEPS, 128), F32),
                *side_scratch * 4,
                pltpu.VMEM((KB * SCORE_BLOCKS, 128), F32),
                pltpu.SMEM((1, 128), jnp.int32),
                pltpu.SMEM((16, 128), jnp.int32),
                pltpu.SMEM((2, 128), jnp.int32),
                pltpu.SemaphoreType.DMA((2,)),
                pltpu.SemaphoreType.DMA((2,)),
                pltpu.SemaphoreType.DMA((2,)),
                pltpu.SemaphoreType.DMA((HUBS,)),
                pltpu.SemaphoreType.DMA((16,)),
                pltpu.SemaphoreType.DMA((HUBS,)),
                pltpu.SemaphoreType.DMA((2 * max(map(len, SERVES)),)),
                pltpu.SemaphoreType.DMA((2,)),
                pltpu.SemaphoreType.REGULAR((2,)),
            ],
            compiler_params=pltpu.CompilerParams(collective_id=0, has_side_effects=True),
            name="profile_rows",
        )(
            series.reshape(SEG, 128),
            tail.reshape(M // 128, 128),
            diag_offsets,
            exclusion,
        )
        return rows.reshape(-1)

    in_specs = (P("tm"), P(), P("diag"), P())
    out_specs = P(("tm", "diag"))
    return jax.shard_map(
        on_device, mesh=mesh, in_specs=in_specs, out_specs=out_specs, check_vma=False
    )
```

```python
import functools

import jax
import jax.numpy as jnp
from jax import lax
from jax.experimental import pallas as pl
from jax.experimental.pallas import tpu as pltpu
from jax.sharding import PartitionSpec as P

F32 = jnp.float32
BF16 = jnp.bfloat16
MESH = pl.DeviceIdType.MESH

M = 256
KB = 32
LANES = 128
FILL = 1e30
NOWHERE = 1 << 30

HALO = 96
SEG = 128
OWN = 8
REGION = 2 * HALO + OWN + 16
SKEWED = REGION - 8
EXT = 2 * HALO + SEG + 16
STEPS = KB // 8
SCORE_BLOCKS = OWN + 1

HUBS = 4
SERVES = ((), (0, 10, 11, 12, 13, 14, 15), (6, 7), (4, 5, 8, 9))


def split2(v):
    high = v.astype(BF16)
    return high, (v - high.astype(F32)).astype(BF16)


def window_weights():
    r = lax.broadcasted_iota(jnp.int32, (256, 256), 0) & 127
    c = lax.broadcasted_iota(jnp.int32, (256, 256), 1)
    from_c = jnp.where(r >= c, 1.0, 0.0)
    before_c = jnp.where(r < c - 128, 1.0, 0.0)
    return jnp.where(c < 128, from_c, before_c).astype(BF16)


def window_stats(x_ref, w_ref, mean_ref, a_ref, b_ref):
    def window_sums(v):
        high, mid = split2(v)
        low = (v - high.astype(F32) - mid.astype(F32)).astype(BF16)
        g = jnp.dot(jnp.concatenate([high, mid], axis=1), w_ref[...], preferred_element_type=F32)
        g = g + jnp.dot(low, w_ref[:128, :], preferred_element_type=F32)
        from_c, before_c = g[:, :128], g[:, 128:]
        n = v.shape[0]
        return from_c[: n - 2] + (from_c + before_c)[1 : n - 1] + before_c[2:]

    x = x_ref[...]
    n = x.shape[0] - 2
    first = window_sums(x) * (1.0 / M)
    second = window_sums(x * x) * (1.0 / M)
    spread = 1.0 / jnp.sqrt(second - first * first + 1e-5)
    mean_ref[:n, :] = first
    a_ref[:n, :] = spread * (1.0 / M)
    b_ref[:n, :] = first * spread


def own_rows(ref, out_ref):
    n = 16
    here = ref[HALO : HALO + n, :]
    before = ref[HALO - 1 : HALO - 1 + n, :]
    lanes = lax.broadcasted_iota(jnp.int32, (n, 128), 1)
    out_ref[:n, :] = here
    for v in range(1, STEPS):
        shift = 8 * v
        out_ref[n * v : n * v + n, :] = jnp.where(
            lanes < shift, pltpu.roll(before, shift, 1), pltpu.roll(here, shift, 1)
        )


def skewed(pairs):
    lanes = lax.broadcasted_iota(jnp.int32, (8, 128), 1)
    subs = lax.broadcasted_iota(jnp.int32, (8, 128), 0)
    here = lanes < 121 + subs
    batch = SKEWED // 4

    def rows(i, carry):
        start = batch * i
        for ref, out_ref in pairs:
            last = None
            for j in range(batch + 1):
                row = jnp.broadcast_to(ref[pl.ds(start + j, 1), :], (8, 128))
                rolled = pltpu.roll(row, 121, 1, stride=1, stride_axis=0)
                if j:
                    out_ref[pl.ds(pl.multiple_of(8 * (start + j - 1), 8), 8), :] = jnp.where(here, last, rolled)
                last = rolled
        return carry

    lax.fori_loop(0, SKEWED // batch, rows, 0)


def hankel(ref, row, lane, blocks, emit):
    lanes = lax.broadcasted_iota(jnp.int32, (8, 128), 1)
    here = lanes < 128 - lane
    shift = (128 - lane) & 127
    rolled = [
        pltpu.roll(ref[pl.ds(8 * row + 8 * j, 8), :], shift, 1) for j in range(blocks + 1)
    ]
    for j in range(blocks):
        emit(j, jnp.where(here, rolled[j], rolled[j + 1]))


def group_scores(
    firsts, exclusion, pos0, total, x_ref, a_ref, b_ref, own_x, own_mean, w_ref, scratch, best
):
    subs = lax.broadcasted_iota(jnp.int32, (8, 128), 0)
    lanes = lax.broadcasted_iota(jnp.int32, (8, 128), 1)

    def rows_of(ref, v, j):
        return jnp.broadcast_to(ref[16 * v + j : 16 * v + j + 1, :], (8, 128))

    def at(j, v):
        return slice((STEPS * j + v) * 8, (STEPS * j + v) * 8 + 8)

    sides = []
    for first in firsts:
        for ahead in (True, False):
            beta = first if ahead else -first - (KB - 1)
            start = HALO * 128 + beta
            sides.append((ahead, beta, lax.shift_right_arithmetic(start, 7), start & 127))

    for (_, _, row, lane), (lhs, _) in zip(sides, scratch):

        def emit_products(j, y, lhs=lhs):
            own = jnp.concatenate([rows_of(own_x, v, j) for v in range(STEPS)], axis=0)
            p = jnp.concatenate([y] * STEPS, axis=0) * own
            lhs[KB * j : KB * j + KB, :128] = p
            lhs[KB * j : KB * j + KB, 128:] = p - p.astype(BF16).astype(F32)

        hankel(x_ref, row, lane, SCORE_BLOCKS + 2, emit_products)

    for lhs, sums in scratch[: len(sides)]:
        sums[...] = jnp.dot(lhs[...], w_ref[...], preferred_element_type=F32)

    masks, scaled, shifted = [], [], []
    for ahead, beta, row, lane in sides:
        distance = beta + 7 - subs
        masks.append((
            pos0 + distance + lanes,
            [
                jnp.where(distance + 8 * v >= exclusion, pos0 + distance + lanes, NOWHERE)
                if ahead
                else jnp.where(-8 * v - distance >= exclusion, pos0 + distance + lanes, -NOWHERE)
                for v in range(STEPS)
            ],
        ))
        scaled.append({})
        hankel(a_ref, row, lane, SCORE_BLOCKS, scaled[-1].__setitem__)
        shifted.append({})
        hankel(b_ref, row, lane, SCORE_BLOCKS, shifted[-1].__setitem__)

    for j in range(SCORE_BLOCKS):
        for v in range(STEPS):
            here, middle, after = at(j, v), at(j + 1, v), at(j + 2, v)
            mean = rows_of(own_mean, v, j)
            top = best[here, :]
            for i in range(len(sides)):
                sums = scratch[i][1]
                products = sums[here, :128] + (sums[middle, :128] + sums[middle, 128:]) + sums[after, 128:]
                score = products * scaled[i][j] - mean * shifted[i][j]
                partner = masks[i][1][v]
                counted = partner < total - 128 * j if sides[i][0] else partner >= -128 * j
                top = jnp.maximum(top, jnp.where(counted, score, -FILL))
            best[here, :] = top


def finish(best, a_ref, out_ref):
    def part(j, v):
        return best[(STEPS * j + v) * 8 : (STEPS * j + v) * 8 + 8, :]

    lanes = lax.broadcasted_iota(jnp.int32, (8, 128), 1)
    tops = [part(j, 0) for j in range(OWN)]
    for v in range(1, STEPS):
        moved = [pltpu.roll(part(j, v), 128 - 8 * v, 1) for j in range(SCORE_BLOCKS)]
        for j in range(OWN):
            tops[j] = jnp.maximum(tops[j], jnp.where(lanes < 128 - 8 * v, moved[j], moved[j + 1]))
    top = jnp.concatenate([jnp.max(t, axis=0, keepdims=True) for t in tops], axis=0)
    corr = top * (a_ref[HALO : HALO + OWN, :] * float(M))
    out_ref[...] = jnp.where(top < -0.1 * FILL, FILL, jnp.sqrt(1.0 - corr))


def kernel(
    series_hbm, tail_hbm, offset, exclusion, out,
    series, tail,
    ext, x_ref, mean_ref, a_ref, b_ref, w_ref, ones_ref,
    x_skew, a_skew, b_skew, own_x, own_mean,
    lhs0, sums0, lhs1, sums1, lhs2, sums2, lhs3, sums3, best,
    mine, table, packed, load_sem, halo_send, halo_recv, row_send, row_recv, reply_send, table_send, table_recv, answer,
    *, n_tm, n_diag, total,
):
    tm = lax.axis_index("tm")
    z = lax.axis_index("diag")
    has_prev = tm > 0
    has_next = tm < n_tm - 1

    late = tm == 0
    is_hub = (z < HUBS) & jnp.logical_not(late & (z == 0))
    served_zero = late & (z == 0)

    barrier = pltpu.get_barrier_semaphore()

    answers = lax.rem(tm, 2) == 1

    @pl.when(jnp.logical_not(answers) & has_prev)
    def _():
        pl.semaphore_signal(barrier, inc=1, device_id=(tm - 1, z), device_id_type=MESH)

    @pl.when(jnp.logical_not(answers) & has_next)
    def _():
        pl.semaphore_signal(barrier, inc=1, device_id=(tm + 1, z), device_id_type=MESH)

    for b in range(n_diag - 1, 0, -1):

        @pl.when(is_hub & (z < b))
        def _(b=b):
            pl.semaphore_signal(barrier, inc=1, device_id=(tm, b), device_id_type=MESH)

    @pl.when(is_hub & late)
    def _():
        pl.semaphore_signal(barrier, inc=1, device_id=(tm, 0), device_id_type=MESH)

    mine[0, 0] = offset[0]

    @pl.when(is_hub)
    def _():
        table[z, 0] = offset[0]

    loads = [
        pltpu.make_async_copy(source, target, load_sem.at[i])
        for i, (source, target) in enumerate(
            ((series_hbm, series), (tail_hbm, tail))
        )
    ]
    for load in loads:
        load.start()

    def row_copy(to, send_sem):
        return pltpu.make_async_remote_copy(
            mine, table.at[pl.ds(z, 1)], send_sem, row_recv.at[z], device_id=(tm, to), device_id_type=MESH
        )

    def wait_row(b):
        pltpu.make_async_remote_copy(
            mine, table.at[pl.ds(b, 1)], row_send.at[0], row_recv.at[b], device_id=(tm, 0), device_id_type=MESH
        ).wait_recv()

    def sends_to(a):
        return (z > a) & jnp.logical_not(late) if a == 0 else (z > a) | served_zero

    half = n_diag // 2

    def table_copy(to, i, part):
        rows = packed.at[pl.ds(part, 1)]
        return pltpu.make_async_remote_copy(
            rows, rows, table_send.at[2 * i + part], table_recv.at[part], device_id=(tm, to), device_id_type=MESH
        )

    to_prev = pltpu.make_async_remote_copy(
        series.at[pl.ds(0, HALO)], ext.at[pl.ds(HALO + SEG, HALO)], halo_send.at[0], halo_recv.at[0],
        device_id=(tm - 1, z), device_id_type=MESH,
    )
    to_next = pltpu.make_async_remote_copy(
        series.at[pl.ds(SEG - HALO, HALO)], ext.at[pl.ds(0, HALO)], halo_send.at[1], halo_recv.at[1],
        device_id=(tm + 1, z), device_id_type=MESH,
    )

    edge = has_prev.astype(jnp.int32) + has_next.astype(jnp.int32)
    hubs_below = jnp.where(served_zero, HUBS - 1, jnp.minimum(z, HUBS) - (late & (z > 0)).astype(jnp.int32))
    announced = hubs_below + edge * lax.rem(tm, 2)

    @pl.when(announced > 0)
    def _():
        pl.semaphore_wait(barrier, announced)

    @pl.when(answers & has_prev)
    def _():
        pl.semaphore_signal(answer.at[1], inc=1, device_id=(tm - 1, z), device_id_type=MESH)

    @pl.when(answers & has_next)
    def _():
        pl.semaphore_signal(answer.at[0], inc=1, device_id=(tm + 1, z), device_id_type=MESH)

    for a in range(HUBS):

        @pl.when(sends_to(a))
        def _(a=a):
            row_copy(a, row_send.at[a]).start()

    for load in loads:
        load.wait()

    @pl.when(has_prev)
    def _():
        @pl.when(jnp.logical_not(answers))
        def _():
            pl.semaphore_wait(answer.at[0], 1)

        to_prev.start()

    @pl.when(has_next)
    def _():
        @pl.when(jnp.logical_not(answers))
        def _():
            pl.semaphore_wait(answer.at[1], 1)

        to_next.start()

    ext[HALO : HALO + SEG, :] = series[...]
    ext[2 * HALO + SEG :, :] = jnp.zeros((EXT - 2 * HALO - SEG, 128), F32)

    @pl.when(jnp.logical_not(has_prev))
    def _():
        ext[:HALO, :] = jnp.zeros((HALO, 128), F32)

    @pl.when(jnp.logical_not(has_next))
    def _():
        ext[HALO + SEG : HALO + SEG + 2, :] = tail[...]
        ext[HALO + SEG + 2 : 2 * HALO + SEG, :] = jnp.zeros((HALO - 2, 128), F32)

    w_ref[...] = window_weights()
    ones_ref[...] = w_ref[...].astype(F32)
    scratch = ((lhs0, sums0), (lhs1, sums1), (lhs2, sums2), (lhs3, sums3))
    best[...] = jnp.full(best.shape, -FILL, F32)

    @pl.when(has_next)
    def _():
        to_prev.wait_recv()

    @pl.when(has_prev)
    def _():
        to_next.wait_recv()

    x_ref[...] = ext[pl.ds(pl.multiple_of(OWN * z, OWN), REGION), :]
    window_stats(x_ref, w_ref, mean_ref, a_ref, b_ref)
    skewed(((x_ref, x_skew), (a_ref, a_skew), (b_ref, b_skew)))
    own_rows(x_ref, own_x)
    own_rows(mean_ref, own_mean)
    pos0 = (tm * SEG + z * OWN) * 128

    for b in range(1, HUBS):

        @pl.when(is_hub & (z < b))
        def _(b=b):
            wait_row(b)
            row_copy(b, reply_send.at[b]).start()

    for a in range(HUBS - 1):

        @pl.when(is_hub & (z > a))
        def _(a=a):
            wait_row(a)

    @pl.when(is_hub)
    def _():
        for b in range(HUBS, half):
            wait_row(b)

        for b in range(half):
            packed[0, b] = table[b, 0]

    for hub, served in enumerate(SERVES):

        @pl.when(z == hub)
        def _(served=served):
            for i, to in enumerate(served):
                if to < half:

                    @pl.when(late | (to > 0))
                    def _(i=i, to=to):
                        table_copy(to, i, 0).start()

    @pl.when(jnp.logical_not(is_hub))
    def _():
        table_copy(0, 0, 0).wait_recv()

    def pair(t, carry):
        @pl.when(jnp.logical_not(is_hub) & (t == half // 2))
        def _():
            table_copy(0, 0, 1).wait_recv()

        def take_row(b):
            wait_row(b)
            packed[1, b - half] = table[b, 0]

        for hub, served in enumerate(SERVES):
            if not served:
                for q in range(half // 2):

                    @pl.when(is_hub & (z == hub) & (t == half // 2 + q))
                    def _(q=q):
                        take_row(n_diag - 1 - 2 * q)
                        take_row(n_diag - 2 - 2 * q)

                continue

            @pl.when((z == hub) & (t == half // 2))
            def _(served=served):
                for i, to in enumerate(served):
                    if to >= half:
                        take_row(to)
                        table_copy(to, i, 0).start()
                for b in range(half, n_diag):
                    if b not in served:
                        take_row(b)
                for i, to in enumerate(served):

                    @pl.when(late | (to > 0))
                    def _(i=i, to=to):
                        table_copy(to, i, 1).start()

        part = jnp.where(t < half // 2, 0, 1)
        column = jnp.where(t < half // 2, 2 * t, 2 * (n_diag - half // 2 - 1 - t - half // 2))
        group_scores(
            (packed[part, column], packed[part, column + 1]), exclusion[0], pos0, total,
            x_skew, a_skew, b_skew, own_x, own_mean, ones_ref, scratch, best,
        )
        return carry

    lax.fori_loop(0, n_diag // 2, pair, 0)
    finish(best, a_ref, out)

    for a in range(HUBS):

        @pl.when(sends_to(a))
        def _(a=a):
            row_copy(a, row_send.at[a]).wait_send()

    for b in range(1, HUBS):

        @pl.when(is_hub & (z < b))
        def _(b=b):
            row_copy(b, reply_send.at[b]).wait_send()

    for hub, served in enumerate(SERVES):

        @pl.when(z == hub)
        def _(served=served):
            for i, to in enumerate(served):

                @pl.when(late | (to > 0))
                def _(i=i, to=to):
                    table_copy(to, i, 0).wait_send()
                    table_copy(to, i, 1).wait_send()

    @pl.when(has_prev)
    def _():
        to_prev.wait_send()

    @pl.when(has_next)
    def _():
        to_next.wait_send()


def solution(mesh):
    n_tm, n_diag = mesh.shape["tm"], mesh.shape["diag"]

    def on_device(series, tail, diag_offsets, exclusion):
        total = series.shape[0] * n_tm
        anywhere = pl.BlockSpec(memory_space=pl.ANY)
        smem = pl.BlockSpec(memory_space=pltpu.SMEM)
        product_rows = KB * (SCORE_BLOCKS + 2)
        side_scratch = [pltpu.VMEM((product_rows, 256), F32)] * 2
        rows = pl.pallas_call(
            functools.partial(kernel, n_tm=n_tm, n_diag=n_diag, total=total),
            out_shape=pltpu.VMEM((OWN, 128), F32),
            in_specs=[anywhere, anywhere, smem, smem],
            out_specs=pl.BlockSpec(memory_space=pltpu.VMEM),
            scratch_shapes=[
                pltpu.VMEM((SEG, 128), F32),
                pltpu.VMEM((M // 128, 128), F32),
                pltpu.VMEM((EXT, 128), F32),
                pltpu.VMEM((REGION, 128), F32),
                pltpu.VMEM((REGION, 128), F32),
                pltpu.VMEM((REGION, 128), F32),
                pltpu.VMEM((REGION, 128), F32),
                pltpu.VMEM((256, 256), BF16),
                pltpu.VMEM((256, 256), F32),
                pltpu.VMEM((8 * SKEWED, 128), F32),
                pltpu.VMEM((8 * SKEWED, 128), F32),
                pltpu.VMEM((8 * SKEWED, 128), F32),
                pltpu.VMEM((16 * STEPS, 128), F32),
                pltpu.VMEM((16 * STEPS, 128), F32),
                *side_scratch * 4,
                pltpu.VMEM((KB * SCORE_BLOCKS, 128), F32),
                pltpu.SMEM((1, 128), jnp.int32),
                pltpu.SMEM((16, 128), jnp.int32),
                pltpu.SMEM((2, 128), jnp.int32),
                pltpu.SemaphoreType.DMA((2,)),
                pltpu.SemaphoreType.DMA((2,)),
                pltpu.SemaphoreType.DMA((2,)),
                pltpu.SemaphoreType.DMA((HUBS,)),
                pltpu.SemaphoreType.DMA((16,)),
                pltpu.SemaphoreType.DMA((HUBS,)),
                pltpu.SemaphoreType.DMA((2 * max(map(len, SERVES)),)),
                pltpu.SemaphoreType.DMA((2,)),
                pltpu.SemaphoreType.REGULAR((2,)),
            ],
            compiler_params=pltpu.CompilerParams(collective_id=0, has_side_effects=True),
            name="profile_rows",
        )(
            series.reshape(SEG, 128),
            tail.reshape(M // 128, 128),
            diag_offsets,
            exclusion,
        )
        return rows.reshape(-1)

    in_specs = (P("tm"), P(), P("diag"), P())
    out_specs = P(("tm", "diag"))
    return jax.shard_map(
        on_device, mesh=mesh, in_specs=in_specs, out_specs=out_specs, check_vma=False
    )
```

```python
import functools

import jax
import jax.numpy as jnp
from jax import lax
from jax.experimental import pallas as pl
from jax.experimental.pallas import tpu as pltpu
from jax.sharding import PartitionSpec as P

F32 = jnp.float32
BF16 = jnp.bfloat16
MESH = pl.DeviceIdType.MESH

M = 256
KB = 32
LANES = 128
FILL = 1e30
NOWHERE = 1 << 30

HALO = 96
SEG = 128
OWN = 8
REGION = 2 * HALO + OWN + 16
SKEWED = REGION - 8
EXT = 2 * HALO + SEG + 16
STEPS = KB // 8
SCORE_BLOCKS = OWN + 1

HUBS = 4
SERVES = ((), (0, 10, 11, 12, 13, 14, 15), (6, 7), (4, 5, 8, 9))


def split2(v):
    high = v.astype(BF16)
    return high, (v - high.astype(F32)).astype(BF16)


def window_weights():
    r = lax.broadcasted_iota(jnp.int32, (256, 256), 0) & 127
    c = lax.broadcasted_iota(jnp.int32, (256, 256), 1)
    from_c = jnp.where(r >= c, 1.0, 0.0)
    before_c = jnp.where(r < c - 128, 1.0, 0.0)
    return jnp.where(c < 128, from_c, before_c).astype(BF16)


def window_stats(x_ref, w_ref, mean_ref, a_ref, b_ref):
    def window_sums(v):
        high, mid = split2(v)
        low = (v - high.astype(F32) - mid.astype(F32)).astype(BF16)
        g = jnp.dot(jnp.concatenate([high, mid], axis=1), w_ref[...], preferred_element_type=F32)
        g = g + jnp.dot(low, w_ref[:128, :], preferred_element_type=F32)
        from_c, before_c = g[:, :128], g[:, 128:]
        n = v.shape[0]
        return from_c[: n - 2] + (from_c + before_c)[1 : n - 1] + before_c[2:]

    x = x_ref[...]
    n = x.shape[0] - 2
    first = window_sums(x) * (1.0 / M)
    second = window_sums(x * x) * (1.0 / M)
    spread = 1.0 / jnp.sqrt(second - first * first + 1e-5)
    mean_ref[:n, :] = first
    a_ref[:n, :] = spread * (1.0 / M)
    b_ref[:n, :] = first * spread


def own_rows(ref, out_ref):
    n = 16
    here = ref[HALO : HALO + n, :]
    before = ref[HALO - 1 : HALO - 1 + n, :]
    lanes = lax.broadcasted_iota(jnp.int32, (n, 128), 1)
    out_ref[:n, :] = here
    for v in range(1, STEPS):
        shift = 8 * v
        out_ref[n * v : n * v + n, :] = jnp.where(
            lanes < shift, pltpu.roll(before, shift, 1), pltpu.roll(here, shift, 1)
        )


def skewed(pairs):
    lanes = lax.broadcasted_iota(jnp.int32, (8, 128), 1)
    subs = lax.broadcasted_iota(jnp.int32, (8, 128), 0)
    here = lanes < 121 + subs
    batch = SKEWED // 4

    def rows(i, carry):
        start = batch * i
        for ref, out_ref in pairs:
            last = None
            for j in range(batch + 1):
                row = jnp.broadcast_to(ref[pl.ds(start + j, 1), :], (8, 128))
                rolled = pltpu.roll(row, 121, 1, stride=1, stride_axis=0)
                if j:
                    out_ref[pl.ds(pl.multiple_of(8 * (start + j - 1), 8), 8), :] = jnp.where(here, last, rolled)
                last = rolled
        return carry

    lax.fori_loop(0, SKEWED // batch, rows, 0)


def hankel(ref, row, lane, blocks, emit):
    lanes = lax.broadcasted_iota(jnp.int32, (8, 128), 1)
    here = lanes < 128 - lane
    shift = (128 - lane) & 127
    rolled = [
        pltpu.roll(ref[pl.ds(8 * row + 8 * j, 8), :], shift, 1) for j in range(blocks + 1)
    ]
    for j in range(blocks):
        emit(j, jnp.where(here, rolled[j], rolled[j + 1]))


def group_scores(
    firsts, exclusion, pos0, total, x_ref, a_ref, b_ref, own_x, own_mean, w_ref, scratch, best
):
    subs = lax.broadcasted_iota(jnp.int32, (8, 128), 0)
    lanes = lax.broadcasted_iota(jnp.int32, (8, 128), 1)

    def rows_of(ref, v, j):
        return jnp.broadcast_to(ref[16 * v + j : 16 * v + j + 1, :], (8, 128))

    def at(j, v):
        return slice((STEPS * j + v) * 8, (STEPS * j + v) * 8 + 8)

    sides = []
    for first in firsts:
        for ahead in (True, False):
            beta = first if ahead else -first - (KB - 1)
            start = HALO * 128 + beta
            sides.append((ahead, beta, lax.shift_right_arithmetic(start, 7), start & 127))

    for (_, _, row, lane), (lhs, _) in zip(sides, scratch):

        def emit_products(j, y, lhs=lhs):
            own = jnp.concatenate([rows_of(own_x, v, j) for v in range(STEPS)], axis=0)
            p = jnp.concatenate([y] * STEPS, axis=0) * own
            lhs[KB * j : KB * j + KB, :128] = p
            lhs[KB * j : KB * j + KB, 128:] = p - p.astype(BF16).astype(F32)

        hankel(x_ref, row, lane, SCORE_BLOCKS + 2, emit_products)

    for lhs, sums in scratch[: len(sides)]:
        sums[...] = jnp.dot(lhs[...], w_ref[...], preferred_element_type=F32)

    masks, scaled, shifted = [], [], []
    for ahead, beta, row, lane in sides:
        distance = beta + 7 - subs
        masks.append((
            pos0 + distance + lanes,
            [
                jnp.where(distance + 8 * v >= exclusion, pos0 + distance + lanes, NOWHERE)
                if ahead
                else jnp.where(-8 * v - distance >= exclusion, pos0 + distance + lanes, -NOWHERE)
                for v in range(STEPS)
            ],
        ))
        scaled.append({})
        hankel(a_ref, row, lane, SCORE_BLOCKS, scaled[-1].__setitem__)
        shifted.append({})
        hankel(b_ref, row, lane, SCORE_BLOCKS, shifted[-1].__setitem__)

    for j in range(SCORE_BLOCKS):
        for v in range(STEPS):
            here, middle, after = at(j, v), at(j + 1, v), at(j + 2, v)
            mean = rows_of(own_mean, v, j)
            top = best[here, :]
            for i in range(len(sides)):
                sums = scratch[i][1]
                products = sums[here, :128] + (sums[middle, :128] + sums[middle, 128:]) + sums[after, 128:]
                score = products * scaled[i][j] - mean * shifted[i][j]
                partner = masks[i][1][v]
                counted = partner < total - 128 * j if sides[i][0] else partner >= -128 * j
                top = jnp.maximum(top, jnp.where(counted, score, -FILL))
            best[here, :] = top


def finish(best, a_ref, out_ref):
    def part(j, v):
        return best[(STEPS * j + v) * 8 : (STEPS * j + v) * 8 + 8, :]

    lanes = lax.broadcasted_iota(jnp.int32, (8, 128), 1)
    tops = [part(j, 0) for j in range(OWN)]
    for v in range(1, STEPS):
        moved = [pltpu.roll(part(j, v), 128 - 8 * v, 1) for j in range(SCORE_BLOCKS)]
        for j in range(OWN):
            tops[j] = jnp.maximum(tops[j], jnp.where(lanes < 128 - 8 * v, moved[j], moved[j + 1]))
    top = jnp.concatenate([jnp.max(t, axis=0, keepdims=True) for t in tops], axis=0)
    corr = top * (a_ref[HALO : HALO + OWN, :] * float(M))
    out_ref[...] = jnp.where(top < -0.1 * FILL, FILL, jnp.sqrt(1.0 - corr))


def kernel(
    series_hbm, tail_hbm, offset, exclusion, out,
    series, tail,
    ext, x_ref, mean_ref, a_ref, b_ref, w_ref, ones_ref,
    x_skew, a_skew, b_skew, own_x, own_mean,
    lhs0, sums0, lhs1, sums1, lhs2, sums2, lhs3, sums3, best,
    mine, table, packed, load_sem, halo_send, halo_recv, row_send, row_recv, reply_send, table_send, table_recv, answer,
    *, n_tm, n_diag, total,
):
    tm = lax.axis_index("tm")
    z = lax.axis_index("diag")
    has_prev = tm > 0
    has_next = tm < n_tm - 1

    late = tm == 0
    is_hub = (z < HUBS) & jnp.logical_not(late & (z == 0))
    served_zero = late & (z == 0)

    barrier = pltpu.get_barrier_semaphore()

    answers = lax.rem(tm, 2) == 1

    @pl.when(jnp.logical_not(answers) & has_prev)
    def _():
        pl.semaphore_signal(barrier, inc=1, device_id=(tm - 1, z), device_id_type=MESH)

    @pl.when(jnp.logical_not(answers) & has_next)
    def _():
        pl.semaphore_signal(barrier, inc=1, device_id=(tm + 1, z), device_id_type=MESH)

    @pl.when(is_hub)
    def _():
        for b in range(n_diag - 1, 0, -1):

            @pl.when(z < b)
            def _(b=b):
                pl.semaphore_signal(barrier, inc=1, device_id=(tm, b), device_id_type=MESH)

    @pl.when(is_hub & late)
    def _():
        pl.semaphore_signal(barrier, inc=1, device_id=(tm, 0), device_id_type=MESH)

    mine[0, 0] = offset[0]

    @pl.when(is_hub)
    def _():
        table[z, 0] = offset[0]

    loads = [
        pltpu.make_async_copy(source, target, load_sem.at[i])
        for i, (source, target) in enumerate(
            ((series_hbm, series), (tail_hbm, tail))
        )
    ]
    for load in loads:
        load.start()

    def row_copy(to, send_sem):
        return pltpu.make_async_remote_copy(
            mine, table.at[pl.ds(z, 1)], send_sem, row_recv.at[z], device_id=(tm, to), device_id_type=MESH
        )

    def wait_row(b):
        pltpu.make_async_remote_copy(
            mine, table.at[pl.ds(b, 1)], row_send.at[0], row_recv.at[b], device_id=(tm, 0), device_id_type=MESH
        ).wait_recv()

    def sends_to(a):
        return (z > a) & jnp.logical_not(late) if a == 0 else (z > a) | served_zero

    half = n_diag // 2

    def table_copy(to, i, part):
        rows = packed.at[pl.ds(part, 1)]
        return pltpu.make_async_remote_copy(
            rows, rows, table_send.at[2 * i + part], table_recv.at[part], device_id=(tm, to), device_id_type=MESH
        )

    to_prev = pltpu.make_async_remote_copy(
        series.at[pl.ds(0, HALO)], ext.at[pl.ds(HALO + SEG, HALO)], halo_send.at[0], halo_recv.at[0],
        device_id=(tm - 1, z), device_id_type=MESH,
    )
    to_next = pltpu.make_async_remote_copy(
        series.at[pl.ds(SEG - HALO, HALO)], ext.at[pl.ds(0, HALO)], halo_send.at[1], halo_recv.at[1],
        device_id=(tm + 1, z), device_id_type=MESH,
    )

    edge = has_prev.astype(jnp.int32) + has_next.astype(jnp.int32)
    hubs_below = jnp.where(served_zero, HUBS - 1, jnp.minimum(z, HUBS) - (late & (z > 0)).astype(jnp.int32))
    announced = hubs_below + edge * lax.rem(tm, 2)

    @pl.when(announced > 0)
    def _():
        pl.semaphore_wait(barrier, announced)

    @pl.when(answers & has_prev)
    def _():
        pl.semaphore_signal(answer.at[1], inc=1, device_id=(tm - 1, z), device_id_type=MESH)

    @pl.when(answers & has_next)
    def _():
        pl.semaphore_signal(answer.at[0], inc=1, device_id=(tm + 1, z), device_id_type=MESH)

    for a in range(HUBS):

        @pl.when(sends_to(a))
        def _(a=a):
            row_copy(a, row_send.at[a]).start()

    for load in loads:
        load.wait()

    @pl.when(has_prev)
    def _():
        @pl.when(jnp.logical_not(answers))
        def _():
            pl.semaphore_wait(answer.at[0], 1)

        to_prev.start()

    @pl.when(has_next)
    def _():
        @pl.when(jnp.logical_not(answers))
        def _():
            pl.semaphore_wait(answer.at[1], 1)

        to_next.start()

    ext[HALO : HALO + SEG, :] = series[...]
    ext[2 * HALO + SEG :, :] = jnp.zeros((EXT - 2 * HALO - SEG, 128), F32)

    @pl.when(jnp.logical_not(has_prev))
    def _():
        ext[:HALO, :] = jnp.zeros((HALO, 128), F32)

    @pl.when(jnp.logical_not(has_next))
    def _():
        ext[HALO + SEG : HALO + SEG + 2, :] = tail[...]
        ext[HALO + SEG + 2 : 2 * HALO + SEG, :] = jnp.zeros((HALO - 2, 128), F32)

    w_ref[...] = window_weights()
    ones_ref[...] = w_ref[...].astype(F32)
    scratch = ((lhs0, sums0), (lhs1, sums1), (lhs2, sums2), (lhs3, sums3))
    best[...] = jnp.full(best.shape, -FILL, F32)

    @pl.when(has_next)
    def _():
        to_prev.wait_recv()

    @pl.when(has_prev)
    def _():
        to_next.wait_recv()

    x_ref[...] = ext[pl.ds(pl.multiple_of(OWN * z, OWN), REGION), :]
    window_stats(x_ref, w_ref, mean_ref, a_ref, b_ref)
    skewed(((x_ref, x_skew), (a_ref, a_skew), (b_ref, b_skew)))
    own_rows(x_ref, own_x)
    own_rows(mean_ref, own_mean)
    pos0 = (tm * SEG + z * OWN) * 128

    for b in range(1, HUBS):

        @pl.when(is_hub & (z < b))
        def _(b=b):
            wait_row(b)
            row_copy(b, reply_send.at[b]).start()

    for a in range(HUBS - 1):

        @pl.when(is_hub & (z > a))
        def _(a=a):
            wait_row(a)

    @pl.when(is_hub)
    def _():
        for b in range(HUBS, half):
            wait_row(b)

        for b in range(half):
            packed[0, b] = table[b, 0]

    for hub, served in enumerate(SERVES):

        @pl.when(z == hub)
        def _(served=served):
            for i, to in enumerate(served):
                if to < half:

                    @pl.when(late | (to > 0))
                    def _(i=i, to=to):
                        table_copy(to, i, 0).start()

    @pl.when(jnp.logical_not(is_hub))
    def _():
        table_copy(0, 0, 0).wait_recv()

    def pair(t, carry):
        @pl.when(jnp.logical_not(is_hub) & (t == half // 2))
        def _():
            table_copy(0, 0, 1).wait_recv()

        def take_row(b):
            wait_row(b)
            packed[1, b - half] = table[b, 0]

        for hub, served in enumerate(SERVES):
            if not served:
                for q in range(half // 2):

                    @pl.when(is_hub & (z == hub) & (t == half // 2 + q))
                    def _(q=q):
                        take_row(n_diag - 1 - 2 * q)
                        take_row(n_diag - 2 - 2 * q)

                continue

            @pl.when((z == hub) & (t == half // 2))
            def _(served=served):
                for i, to in enumerate(served):
                    if to >= half:
                        take_row(to)
                        table_copy(to, i, 0).start()
                for b in range(half, n_diag):
                    if b not in served:
                        take_row(b)
                for i, to in enumerate(served):

                    @pl.when(late | (to > 0))
                    def _(i=i, to=to):
                        table_copy(to, i, 1).start()

        part = jnp.where(t < half // 2, 0, 1)
        column = jnp.where(t < half // 2, 2 * t, 2 * (n_diag - half // 2 - 1 - t - half // 2))
        group_scores(
            (packed[part, column], packed[part, column + 1]), exclusion[0], pos0, total,
            x_skew, a_skew, b_skew, own_x, own_mean, ones_ref, scratch, best,
        )
        return carry

    lax.fori_loop(0, n_diag // 2, pair, 0)
    finish(best, a_ref, out)

    for a in range(HUBS):

        @pl.when(sends_to(a))
        def _(a=a):
            row_copy(a, row_send.at[a]).wait_send()

    for b in range(1, HUBS):

        @pl.when(is_hub & (z < b))
        def _(b=b):
            row_copy(b, reply_send.at[b]).wait_send()

    for hub, served in enumerate(SERVES):

        @pl.when(z == hub)
        def _(served=served):
            for i, to in enumerate(served):

                @pl.when(late | (to > 0))
                def _(i=i, to=to):
                    table_copy(to, i, 0).wait_send()
                    table_copy(to, i, 1).wait_send()

    @pl.when(has_prev)
    def _():
        to_prev.wait_send()

    @pl.when(has_next)
    def _():
        to_next.wait_send()


def solution(mesh):
    n_tm, n_diag = mesh.shape["tm"], mesh.shape["diag"]

    def on_device(series, tail, diag_offsets, exclusion):
        total = series.shape[0] * n_tm
        anywhere = pl.BlockSpec(memory_space=pl.ANY)
        smem = pl.BlockSpec(memory_space=pltpu.SMEM)
        product_rows = KB * (SCORE_BLOCKS + 2)
        side_scratch = [pltpu.VMEM((product_rows, 256), F32)] * 2
        rows = pl.pallas_call(
            functools.partial(kernel, n_tm=n_tm, n_diag=n_diag, total=total),
            out_shape=pltpu.VMEM((OWN, 128), F32),
            in_specs=[anywhere, anywhere, smem, smem],
            out_specs=pl.BlockSpec(memory_space=pltpu.VMEM),
            scratch_shapes=[
                pltpu.VMEM((SEG, 128), F32),
                pltpu.VMEM((M // 128, 128), F32),
                pltpu.VMEM((EXT, 128), F32),
                pltpu.VMEM((REGION, 128), F32),
                pltpu.VMEM((REGION, 128), F32),
                pltpu.VMEM((REGION, 128), F32),
                pltpu.VMEM((REGION, 128), F32),
                pltpu.VMEM((256, 256), BF16),
                pltpu.VMEM((256, 256), F32),
                pltpu.VMEM((8 * SKEWED, 128), F32),
                pltpu.VMEM((8 * SKEWED, 128), F32),
                pltpu.VMEM((8 * SKEWED, 128), F32),
                pltpu.VMEM((16 * STEPS, 128), F32),
                pltpu.VMEM((16 * STEPS, 128), F32),
                *side_scratch * 4,
                pltpu.VMEM((KB * SCORE_BLOCKS, 128), F32),
                pltpu.SMEM((1, 128), jnp.int32),
                pltpu.SMEM((16, 128), jnp.int32),
                pltpu.SMEM((2, 128), jnp.int32),
                pltpu.SemaphoreType.DMA((2,)),
                pltpu.SemaphoreType.DMA((2,)),
                pltpu.SemaphoreType.DMA((2,)),
                pltpu.SemaphoreType.DMA((HUBS,)),
                pltpu.SemaphoreType.DMA((16,)),
                pltpu.SemaphoreType.DMA((HUBS,)),
                pltpu.SemaphoreType.DMA((2 * max(map(len, SERVES)),)),
                pltpu.SemaphoreType.DMA((2,)),
                pltpu.SemaphoreType.REGULAR((2,)),
            ],
            compiler_params=pltpu.CompilerParams(collective_id=0, has_side_effects=True),
            name="profile_rows",
        )(
            series.reshape(SEG, 128),
            tail.reshape(M // 128, 128),
            diag_offsets,
            exclusion,
        )
        return rows.reshape(-1)

    in_specs = (P("tm"), P(), P("diag"), P())
    out_specs = P(("tm", "diag"))
    return jax.shard_map(
        on_device, mesh=mesh, in_specs=in_specs, out_specs=out_specs, check_vma=False
    )
```
